128 devices in a mesh: gx: 4 (over y), gy: 8 (over z, x_hi), gz: 4 (over x_lo, core).
Axes of the slice: x: 4 (x_hi: 2, x_lo: 2; x = x_hi * 2 + x_lo), y: 4, z: 4, core: 2. Of those that a mesh axis runs over, the one named last changes fastest.
Arguments:
- right_side: float32 [64, 1024, 1024], P('gz', 'gx', 'gy'), may hold values from -8 to 8
- diagonal: float32 [64, 1024, 1024], P('gz', 'gx', 'gy'), may hold values from 0.02 to 1
- regime: int32 [1024, 1024], P('gx', 'gy'), may hold values from 0 to 7
- inverses: float32 [8, 64, 64], replicated, as said below
Outputs:
- solution: float32 [64, 1024, 1024], P('gz', 'gx', 'gy')
- residual: float32 [64, 1024, 1024], P('gz', 'gx', 'gy')
The draws below stay inside these ranges and needn't reach their ends.
Inputs may be any that keep to these rules, and one draw needn't show every extreme that they name: `inverses`: each block is symmetric positive definite.
All inputs are finite; a program needn't handle non-finite values.
Results may differ from the reference program's by a relative error of at most 0.00025.
Values sent between devices are 32-bit elements; how exact they have to be, the bound alone decides.
A program may use at most 128 MiB of HBM per device.

```python
import math
import jax
import jax.numpy as jnp
from jax import lax

NZ = 64
NREG = 8
ITERS = 3
NX = 1024
NY = 1024


def draw_inverses(key, part):
    coeffs = jax.random.uniform(key, (NREG, NZ), jnp.float32, 2.3, 4.5)
    upper = jnp.eye(NZ, k=1, dtype=jnp.float32)
    lower = jnp.eye(NZ, k=-1, dtype=jnp.float32)
    tridiag = coeffs[:, :, None] * jnp.eye(NZ, dtype=jnp.float32)[None] - upper[None] - lower[None]
    inverted = jnp.linalg.inv(tridiag)
    return (0.5 * (inverted + jnp.swapaxes(inverted, 1, 2))).astype(jnp.float32)


def touch_ends(entries, rng, low, high):
    dims = entries.shape
    spot = [jax.random.randint(jax.random.fold_in(rng, axis), (), 0, dims[axis]) for axis in range(len(dims))]
    entries = entries.at[tuple(spot)].set(low)
    longest = dims.index(max(dims))
    spot[longest] = (spot[longest] + 1) % dims[longest]
    return entries.at[tuple(spot)].set(high)


def level_of(rng, shape, pieces, least, top_value):
    def one(axis_at, shards_of):
        draws = jax.random.uniform(jax.random.fold_in(jax.random.fold_in(rng, 6), axis_at), (shards_of,), jnp.float32, least / len(pieces), top_value / len(pieces))
        return jnp.repeat(jnp.exp(draws), shape[axis_at] // shards_of).reshape((-1,) + (1,) * (len(shape) - axis_at - 1))

    gain = one(*pieces[0])
    for cut in pieces[1:]:
        gain = gain * one(*cut)
    return gain


def bell_draw(stream_key, shape, deviation, limit, shards=(), kind=jnp.bfloat16):
    entries = jax.random.normal(stream_key, shape, jnp.float32) * deviation
    if len(shards) > 0:
        entries = level_of(stream_key, shape, shards, -0.22, 0.18) * entries
    return jnp.clip(entries, min=-limit, max=limit).astype(kind)


def setup_inputs(seed: int = 0) -> dict:
    arg_keys = jax.random.split(jax.random.key(seed), 5)
    return {
        "right_side": bell_draw(arg_keys[0], (NZ, NX, NY), 1.0, 8.0, ((0, 4), (1, 4), (2, 8)), jnp.float32),
        "diagonal": jnp.clip(jnp.exp(math.log(1.0) - 3.912023 * jax.random.uniform(arg_keys[1], (NZ, NX, NY), jnp.float32) ** level_of(arg_keys[1], (NZ, NX, NY), ((0, 4), (1, 4), (2, 8)), -0.2, 0.2)), 0.02, 1.0),
        "regime": touch_ends(jax.random.randint(arg_keys[2], (NX, NY), 0, NREG), jax.random.fold_in(arg_keys[2], 1), 0, NREG - 1).astype(jnp.int32),
        "inverses": draw_inverses(jax.random.fold_in(arg_keys[4], 71), 0),
    }


def operate(grid_field, diagonal):
    padded = jnp.pad(grid_field, 1)
    beside = padded[2:, 1:-1, 1:-1] + padded[:-2, 1:-1, 1:-1]
    beside = beside + padded[1:-1, 2:, 1:-1] + padded[1:-1, :-2, 1:-1]
    beside = beside + padded[1:-1, 1:-1, 2:] + padded[1:-1, 1:-1, :-2]
    return (6.0 + diagonal) * grid_field - beside

def precondition(grid_field, regime, inverses):
    flattened = grid_field.reshape(grid_field.shape[0], -1)
    chosen = regime.reshape(-1)
    result = jnp.zeros_like(flattened)
    for member in range(NREG):
        product = jnp.dot(inverses[member], flattened, precision=lax.Precision.HIGHEST)
        result = result + jnp.where(chosen[None, :] == member, product, jnp.zeros_like(product))
    return result.reshape(grid_field.shape)

def reference(right_side, diagonal, regime, inverses):
    solution = jnp.zeros_like(right_side)
    residual = right_side
    precond = precondition(residual, regime, inverses)
    inner_rz = jnp.sum(residual * precond)
    search = precond
    for iteration in range(ITERS):
        image = operate(search, diagonal)
        step_len = inner_rz / jnp.sum(search * image)
        solution = solution + step_len * search
        residual = residual - step_len * image
        if iteration + 1 < ITERS:
            precond = precondition(residual, regime, inverses)
            rz_next = jnp.sum(residual * precond)
            search = precond + rz_next / inner_rz * search
            inner_rz = rz_next
    return (solution, residual)
```

```python
import functools

import jax
import jax.numpy as jnp
from jax import lax
from jax.experimental import pallas as pl
from jax.experimental.pallas import tpu as pltpu
from jax.sharding import PartitionSpec as P

f32 = jnp.float32
bf16 = jnp.bfloat16
MESH = pl.DeviceIdType.MESH
NREG = 8
ROWS = 64
DEEP = 64
SLAB = 16
LANES = 128
CHUNK = 16
STEPS = ROWS // CHUNK


def halves(v):
    high = v.astype(bf16)
    return high, (v - high.astype(f32)).astype(bf16)


def tiled(v):
    return v.reshape(DEEP // 8, 8, LANES)


def flat(v):
    return v.reshape(DEEP, LANES)


def kernel(
    right_side, diagonal, regime, blocks,
    out_sol, out_res,
    res, diag, u0, m0, m1, w0, n0, u1, w1, p1, x2, s1, fin, finr,
    reg, inv, stack, edge, left, right, sum_a, sum_b, sum_c,
    col_sem, in_send, small_sem, halo_recv, halo_send, sum_recv, sum_send, out_recv, out_send,
):
    gx, gy, gz = lax.axis_index("gx"), lax.axis_index("gy"), lax.axis_index("gz")
    odd = lax.rem(gx, 2)
    part = gz + odd * (3 - 2 * gz)
    stride = 1 - 2 * odd
    first, last = (3 - part) // 3, part // 3
    line = gx * 4 + part
    lower = {"gx": gx - first, "gz": gz - stride * (1 - first)}
    upper = {"gx": gx + last, "gz": gz + stride * (1 - last)}
    has_lower, has_upper = line > 0, line < 15
    has_left, has_right = gy > 0, gy < 7

    def others(axis, me, count):
        return [{axis: lax.rem(me + j, count)} for j in range(1, count)]

    barrier = pltpu.get_barrier_semaphore()
    peers = others("gz", gz, 4) + others("gx", gx, 4) + others("gy", gy, 8)
    for peer in peers:
        pl.semaphore_signal(barrier, inc=1, device_id=peer, device_id_type=MESH)

    small = [
        pltpu.make_async_copy(blocks, inv, small_sem.at[0]),
        pltpu.make_async_copy(
            regime.at[pl.ds(pl.multiple_of(part * ROWS, ROWS), ROWS), :], reg, small_sem.at[1]
        ),
    ]
    for copy in small:
        copy.start()
    base = pl.multiple_of(gz * SLAB, SLAB)

    def part_of(k):
        return k + odd * (3 - 2 * k)

    def send_columns(array, source, target, c):
        def body(d, carry):
            rows = pl.ds(c * CHUNK, CHUNK)
            for j in range(1, 4):
                k = lax.rem(gz + j, 4)
                begin = pl.multiple_of(part_of(k) * ROWS + c * CHUNK, CHUNK)
                pltpu.make_async_remote_copy(
                    source.at[d, pl.ds(begin, CHUNK), :],
                    target.at[rows, base + d, :],
                    in_send.at[array],
                    col_sem.at[array, c],
                    device_id={"gz": k},
                    device_id_type=MESH,
                ).start()
            begin = pl.multiple_of(part * ROWS + c * CHUNK, CHUNK)
            pltpu.make_async_copy(
                source.at[d, pl.ds(begin, CHUNK), :],
                target.at[rows, base + d, :],
                col_sem.at[array, c],
            ).start()
            return carry

        lax.fori_loop(0, SLAB, body, 0)

    pl.semaphore_wait(barrier, 13)
    for c in range(STEPS):
        send_columns(0, right_side, res, c)
    for c in range(STEPS // 2):
        send_columns(1, diagonal, diag, c)

    nothing = jnp.zeros((DEEP, LANES), f32)
    for array in (u0, m0, m1):

        @pl.when(line == 0)
        def _():
            array[0] = nothing

        @pl.when(line == 15)
        def _():
            array[ROWS + 1] = nothing

    for it in range(3):

        @pl.when(gy == 0)
        def _():
            left[it] = nothing

        @pl.when(gy == 7)
        def _():
            right[it] = nothing

        edge[it, 0] = nothing
        edge[it, 1] = nothing

    for copy in small:
        copy.wait()
    high, low = halves(inv[...])
    stack[...] = jnp.concatenate([high, high, low, low], axis=1)

    lane = lax.broadcasted_iota(jnp.int32, (DEEP, LANES), 1)

    def apply_blocks(source, target, it, c):
        to_left, to_right = edge[it, 0], edge[it, 1]
        for h in range(CHUNK // 2):
            x = c * CHUNK + 2 * h
            both = jnp.concatenate([source[x], source[x + 1]], axis=1)
            high, low = halves(both)
            out = jnp.dot(
                stack[...],
                jnp.concatenate([high, low, high, low], axis=0),
                preferred_element_type=f32,
            )
            kind = jnp.concatenate([reg[pl.ds(x, 1), :], reg[pl.ds(x + 1, 1), :]], axis=1)
            kind = jnp.broadcast_to(kind, (DEEP, 2 * LANES))
            some = [out[k * DEEP : (k + 1) * DEEP] for k in range(NREG)]
            for bit in range(3):
                chosen = (kind & (1 << bit)) != 0
                some = [jnp.where(chosen, some[i + 1], some[i]) for i in range(0, len(some), 2)]
            for j in range(2):
                z = some[0][:, j * LANES : (j + 1) * LANES]
                target[x + j + 1] = z
                here = lane == x + j
                to_left = jnp.where(here, pltpu.roll(z, x + j, 1), to_left)
                to_right = jnp.where(here, pltpu.roll(z, x + j + 1, 1), to_right)
        edge[it, 0] = to_left
        edge[it, 1] = to_right

    def halo_copies(array, it):
        def copy(k, source, target, device):
            return pltpu.make_async_remote_copy(
                source, target, halo_send.at[it, k], halo_recv.at[it, k],
                device_id=device, device_id_type=MESH,
            )

        return (
            (has_lower, has_upper, copy(0, array.at[1], array.at[ROWS + 1], lower)),
            (has_upper, has_lower, copy(1, array.at[ROWS], array.at[0], upper)),
            (has_left, has_right, copy(2, edge.at[it, 0], right.at[it], {"gy": gy - 1})),
            (has_right, has_left, copy(3, edge.at[it, 1], left.at[it], {"gy": gy + 1})),
        )

    def start_halo(array, it):
        for sends, _, copy in halo_copies(array, it):
            pl.when(sends)(copy.start)

    def wait_halo(array, it):
        for _, receives, copy in halo_copies(array, it):
            pl.when(receives)(copy.wait_recv)

    def stencil(array, it, x):
        v = array[x + 1]
        beside = array[x] + array[x + 2]
        empty = jnp.zeros((1, LANES), f32)
        beside = beside + jnp.concatenate([empty, v[:-1]], axis=0)
        beside = beside + jnp.concatenate([v[1:], empty], axis=0)
        from_left = pltpu.roll(left[it], lax.rem(LANES - x, LANES), 1)
        from_right = pltpu.roll(right[it], LANES - 1 - x, 1)
        beside = beside + jnp.where(lane == 0, from_left, pltpu.roll(v, 1, 1))
        beside = beside + jnp.where(lane == LANES - 1, from_right, pltpu.roll(v, LANES - 1, 1))
        return v, (6.0 + diag[x]) * v - beside

    sums = ((sum_a, "gz", gz, 4), (sum_b, "gx", gx, 4), (sum_c, "gy", gy, 8))

    def start_sum(it, stage, value):
        buffer, axis, me, count = sums[stage]
        buffer[it, me] = value
        for peer in others(axis, me, count):
            pltpu.make_async_remote_copy(
                buffer.at[it, me], buffer.at[it, me], sum_send.at[it, stage], sum_recv.at[it, stage],
                device_id=peer, device_id_type=MESH,
            ).start()

    def end_sum(it, stage):
        buffer, _, _, count = sums[stage]
        some = buffer.at[it, pl.ds(0, count - 1)]
        pltpu.make_async_copy(some, some, sum_recv.at[it, stage]).wait()
        total = buffer[it, 0]
        for k in range(1, count):
            total = total + buffer[it, k]
        return total

    def totals(it):
        total = end_sum(it, 2)
        whole = [jnp.sum(total[k], keepdims=True) for k in range(2)]
        return [jnp.broadcast_to(t, (8, LANES)) for t in whole]

    def folded(v):
        return jnp.sum(tiled(v), axis=0)

    def rows_of(c, body, carry):
        return lax.fori_loop(c * CHUNK, (c + 1) * CHUNK, body, carry)

    zero = jnp.zeros((8, LANES), f32)

    def first_precond(c, carry):
        some = res.at[pl.ds(pl.multiple_of(c * CHUNK, CHUNK), CHUNK)]
        pltpu.make_async_copy(some, some, col_sem.at[0, c]).wait()
        apply_blocks(res, u0, 0, c)
        return carry

    lax.fori_loop(0, STEPS, first_precond, 0)
    start_halo(u0, 0)
    for c in range(STEPS // 2, STEPS):
        send_columns(1, diagonal, diag, c)
    wait_halo(u0, 0)

    def first_image(c, carry):
        some = diag.at[pl.ds(pl.multiple_of(c * CHUNK, CHUNK), CHUNK)]
        pltpu.make_async_copy(some, some, col_sem.at[1, c]).wait()

        def body(x, carry):
            rz, wz = carry
            u, w = stencil(u0, 0, x)
            w0[x] = w
            return rz + folded(res[x] * u), wz + folded(w * u)

        return rows_of(c, body, carry)

    rz, wz = lax.fori_loop(0, STEPS, first_image, (zero, zero))

    def blocks_beside_sum(it, source, target):
        def body(c, carry):
            apply_blocks(source, target, it + 1, c)
            for stage in range(2):

                @pl.when(c == 2 * stage)
                def _():
                    start_sum(it, stage + 1, end_sum(it, stage))

            return carry

        lax.fori_loop(0, STEPS, body, 0)

    start_sum(0, 0, jnp.stack([rz, wz]))
    blocks_beside_sum(0, w0, m0)
    start_halo(m0, 1)
    rz0, wz0 = totals(0)
    alpha0 = rz0 / wz0
    wait_halo(m0, 1)

    def second(x, carry):
        rz, wz = carry
        m, n = stencil(m0, 1, x)
        n0[x] = n
        w = w0[x]
        r = flat(tiled(res[x]) - alpha0 * tiled(w))
        u = flat(tiled(u0[x + 1]) - alpha0 * tiled(m))
        w = flat(tiled(w) - alpha0 * tiled(n))
        res[x] = r
        u1[x] = u
        w1[x] = w
        return rz + folded(r * u), wz + folded(w * u)

    rz, wz = lax.fori_loop(0, ROWS, second, (zero, zero))
    start_sum(1, 0, jnp.stack([rz, wz]))
    blocks_beside_sum(1, w1, m1)
    start_halo(m1, 2)
    rz1, wz1 = totals(1)
    beta1 = rz1 / rz0
    alpha1 = rz1 / (wz1 - beta1 * rz1 / alpha0)
    wait_halo(m1, 2)

    def third(x, carry):
        rz, wz = carry
        m, n = stencil(m1, 2, x)
        first_u, first_w = tiled(u0[x + 1]), tiled(w0[x])
        u, w = tiled(u1[x]), tiled(w1[x])
        p = u + beta1 * first_u
        s = w + beta1 * first_w
        r = tiled(res[x]) - alpha1 * s
        u = u - alpha1 * (tiled(m) + beta1 * tiled(m0[x + 1]))
        w = w - alpha1 * (tiled(n) + beta1 * tiled(n0[x]))
        p1[x] = flat(p)
        s1[x] = flat(s)
        x2[x] = flat(alpha0 * first_u + alpha1 * p)
        res[x] = flat(r)
        u1[x] = flat(u)
        w1[x] = flat(w)
        return rz + folded(flat(r * u)), wz + folded(flat(w * u))

    rz, wz = lax.fori_loop(0, ROWS, third, (zero, zero))
    start_sum(2, 0, jnp.stack([rz, wz]))
    start_sum(2, 1, end_sum(2, 0))
    start_sum(2, 2, end_sum(2, 1))
    rz2, wz2 = totals(2)
    beta2 = rz2 / rz1
    alpha2 = rz2 / (wz2 - beta2 * rz2 / alpha1)

    def last_rows(x, carry):
        p = tiled(u1[x]) + beta2 * tiled(p1[x])
        s = tiled(w1[x]) + beta2 * tiled(s1[x])
        fin[x] = flat(tiled(x2[x]) + alpha2 * p)
        finr[x] = flat(tiled(res[x]) - alpha2 * s)
        return carry

    lax.fori_loop(0, ROWS, last_rows, 0)

    mine = pl.ds(pl.multiple_of(part * ROWS, ROWS), ROWS)
    for array, (source, target) in enumerate(((fin, out_sol), (finr, out_res))):

        def send_back(d, carry):
            for j in range(1, 4):
                k = lax.rem(gz + j, 4)
                pltpu.make_async_remote_copy(
                    source.at[:, k * SLAB + d, :],
                    target.at[d, mine, :],
                    out_send.at[array],
                    out_recv.at[array],
                    device_id={"gz": k},
                    device_id_type=MESH,
                ).start()
            pltpu.make_async_copy(
                source.at[:, base + d, :], target.at[d, mine, :], out_recv.at[array]
            ).start()
            return carry

        lax.fori_loop(0, SLAB, send_back, 0)

    for array, target in enumerate((out_sol, out_res)):
        pltpu.make_async_copy(target, target, out_recv.at[array]).wait()
    for array in range(2):
        some = res.at[pl.ds(0, 3 * SLAB)]
        pltpu.make_async_copy(some, some, in_send.at[array]).wait()
        pltpu.make_async_copy(some, some, out_send.at[array]).wait()
    for it, array in enumerate((u0, m0, m1)):
        for sends, _, copy in halo_copies(array, it):
            pl.when(sends)(copy.wait_send)
        for stage, (buffer, _, _, count) in enumerate(sums):
            some = buffer.at[it, pl.ds(0, count - 1)]
            pltpu.make_async_copy(some, some, sum_send.at[it, stage]).wait()


def per_device(right_side, diagonal, regime, inverses):
    shape = jax.ShapeDtypeStruct(right_side.shape, f32)
    field = pltpu.VMEM((ROWS, DEEP, LANES), f32)
    padded = pltpu.VMEM((ROWS + 2, DEEP, LANES), f32)
    plane = (DEEP, LANES)
    return pl.pallas_call(
        kernel,
        out_shape=(shape, shape),
        in_specs=[pl.BlockSpec(memory_space=pl.ANY)] * 4,
        out_specs=[pl.BlockSpec(memory_space=pl.ANY)] * 2,
        scratch_shapes=[field, field, padded, padded, padded] + [field] * 9 + [
            pltpu.VMEM((ROWS, LANES), jnp.int32),
            pltpu.VMEM((NREG * DEEP, DEEP), f32),
            pltpu.VMEM((NREG * DEEP, 4 * DEEP), bf16),
            pltpu.VMEM((3, 2) + plane, f32),
            pltpu.VMEM((3,) + plane, f32),
            pltpu.VMEM((3,) + plane, f32),
            pltpu.VMEM((3, 4, 2, 8, LANES), f32),
            pltpu.VMEM((3, 4, 2, 8, LANES), f32),
            pltpu.VMEM((3, 8, 2, 8, LANES), f32),
            pltpu.SemaphoreType.DMA((2, STEPS)),
            pltpu.SemaphoreType.DMA((2,)),
            pltpu.SemaphoreType.DMA((2,)),
            pltpu.SemaphoreType.DMA((3, 4)),
            pltpu.SemaphoreType.DMA((3, 4)),
            pltpu.SemaphoreType.DMA((3, 3)),
            pltpu.SemaphoreType.DMA((3, 3)),
            pltpu.SemaphoreType.DMA((2,)),
            pltpu.SemaphoreType.DMA((2,)),
        ],
        compiler_params=pltpu.CompilerParams(
            collective_id=0, has_side_effects=True, vmem_limit_bytes=60 * 2**20
        ),
    )(right_side, diagonal, regime, inverses.reshape(NREG * DEEP, DEEP))


def solution(mesh):
    field = P("gz", "gx", "gy")
    return jax.shard_map(
        per_device,
        mesh=mesh,
        in_specs=(field, field, P("gx", "gy"), P()),
        out_specs=(field, field),
        check_vma=False,
    )
```

```python
import functools

import jax
import jax.numpy as jnp
from jax import lax
from jax.experimental import pallas as pl
from jax.experimental.pallas import tpu as pltpu
from jax.sharding import PartitionSpec as P

f32 = jnp.float32
bf16 = jnp.bfloat16
MESH = pl.DeviceIdType.MESH
NREG = 8
ROWS = 64
DEEP = 64
SLAB = 16
LANES = 128
CHUNK = 16
STEPS = ROWS // CHUNK
UNROLL = 8
GROUP = 4


def halves(v):
    high = v.astype(bf16)
    return high, (v - high.astype(f32)).astype(bf16)


def tiled(v):
    return v.reshape(DEEP // 8, 8, LANES)


def flat(v):
    return v.reshape(DEEP, LANES)


def kernel(
    right_side, diagonal, regime, blocks,
    out_sol, out_sides, out_ends,
    res, diag, u0, m0, m1, w0, n0, w1, fin,
    reg, inv, stack, edge, left, right, sides, blank, sum_a, sum_b, sum_c,
    col_sem, in_send, small_sem, halo_recv, halo_send, sum_recv, sum_send, out_recv, sides_recv, ends_recv, out_send,
):
    gx, gy, gz = lax.axis_index("gx"), lax.axis_index("gy"), lax.axis_index("gz")
    odd = lax.rem(gx, 2)
    part = gz + odd * (3 - 2 * gz)
    stride = 1 - 2 * odd
    first, last = (3 - part) // 3, part // 3
    line = gx * 4 + part
    lower = {"gx": gx - first, "gz": gz - stride * (1 - first)}
    upper = {"gx": gx + last, "gz": gz + stride * (1 - last)}
    has_lower, has_upper = line > 0, line < 15
    has_left, has_right = gy > 0, gy < 7

    def others(axis, me, count):
        return [{axis: lax.rem(me + j, count)} for j in range(1, count)]

    barrier = pltpu.get_barrier_semaphore()
    peers = others("gz", gz, 4) + others("gx", gx, 4) + others("gy", gy, 8)
    for peer in peers:
        pl.semaphore_signal(barrier, inc=1, device_id=peer, device_id_type=MESH)

    small = [
        pltpu.make_async_copy(blocks, inv, small_sem.at[0]),
        pltpu.make_async_copy(
            regime.at[pl.ds(pl.multiple_of(part * ROWS, ROWS), ROWS), :], reg, small_sem.at[1]
        ),
    ]
    for copy in small:
        copy.start()
    base = pl.multiple_of(gz * SLAB, SLAB)

    def part_of(k):
        return k + odd * (3 - 2 * k)

    def send_columns(array, source, target, c):
        def body(d, carry):
            rows = pl.ds(c * CHUNK, CHUNK)
            for j in range(1, 4):
                k = lax.rem(gz + j, 4)
                begin = pl.multiple_of(part_of(k) * ROWS + c * CHUNK, CHUNK)
                pltpu.make_async_remote_copy(
                    source.at[d, pl.ds(begin, CHUNK), :],
                    target.at[rows, base + d, :],
                    in_send.at[array],
                    col_sem.at[array, c],
                    device_id={"gz": k},
                    device_id_type=MESH,
                ).start()
            begin = pl.multiple_of(part * ROWS + c * CHUNK, CHUNK)
            pltpu.make_async_copy(
                source.at[d, pl.ds(begin, CHUNK), :],
                target.at[rows, base + d, :],
                col_sem.at[array, c],
            ).start()
            return carry

        lax.fori_loop(0, SLAB, body, 0)

    pl.semaphore_wait(barrier, 13)
    for c in range(STEPS):
        send_columns(0, right_side, res, c)
    for c in range(STEPS // 2):
        send_columns(1, diagonal, diag, c)

    nothing = jnp.zeros((DEEP, LANES), f32)
    blank[...] = nothing
    for array in (u0, m0, m1):

        @pl.when(line == 0)
        def _():
            array[0] = nothing

        @pl.when(line == 15)
        def _():
            array[ROWS + 1] = nothing

    for it in range(3):

        @pl.when(gy == 0)
        def _():
            left[it] = nothing

        @pl.when(gy == 7)
        def _():
            right[it] = nothing

        edge[it, 0] = nothing
        edge[it, 1] = nothing

    for copy in small:
        copy.wait()
    high, low = halves(inv[...])
    stack[...] = jnp.concatenate([high, high, low, low], axis=1)

    lane = lax.broadcasted_iota(jnp.int32, (DEEP, LANES), 1)

    def apply_blocks(source, target, it, c):
        to_left, to_right = edge[it, 0], edge[it, 1]
        for h in range(CHUNK // 2):
            x = c * CHUNK + 2 * h
            both = jnp.concatenate([source[x], source[x + 1]], axis=1)
            high, low = halves(both)
            out = jnp.dot(
                stack[...],
                jnp.concatenate([high, low, high, low], axis=0),
                preferred_element_type=f32,
            )
            kind = jnp.concatenate([reg[pl.ds(x, 1), :], reg[pl.ds(x + 1, 1), :]], axis=1)
            kind = jnp.broadcast_to(kind, (DEEP, 2 * LANES))
            some = [out[k * DEEP : (k + 1) * DEEP] for k in range(NREG)]
            for bit in range(3):
                chosen = (kind & (1 << bit)) != 0
                some = [jnp.where(chosen, some[i + 1], some[i]) for i in range(0, len(some), 2)]
            for j in range(2):
                z = some[0][:, j * LANES : (j + 1) * LANES]
                target[x + j + 1] = z
                here = lane == x + j
                to_left = jnp.where(here, pltpu.roll(z, x + j, 1), to_left)
                to_right = jnp.where(here, pltpu.roll(z, x + j + 1, 1), to_right)
        edge[it, 0] = to_left
        edge[it, 1] = to_right

    def halo_copies(array, it):
        def copy(k, source, target, device):
            return pltpu.make_async_remote_copy(
                source, target, halo_send.at[it, k], halo_recv.at[it, k],
                device_id=device, device_id_type=MESH,
            )

        return (
            (has_lower, has_upper, copy(0, array.at[1], array.at[ROWS + 1], lower)),
            (has_upper, has_lower, copy(1, array.at[ROWS], array.at[0], upper)),
            (has_left, has_right, copy(2, edge.at[it, 0], right.at[it], {"gy": gy - 1})),
            (has_right, has_left, copy(3, edge.at[it, 1], left.at[it], {"gy": gy + 1})),
        )

    def start_halo(array, it):
        for sends, _, copy in halo_copies(array, it):
            pl.when(sends)(copy.start)

    def wait_halo(array, it):
        for _, receives, copy in halo_copies(array, it):
            pl.when(receives)(copy.wait_recv)

    def stencil(array, it, x):
        v = array[x + 1]
        beside = array[x] + array[x + 2]
        empty = jnp.zeros((1, LANES), f32)
        beside = beside + jnp.concatenate([empty, v[:-1]], axis=0)
        beside = beside + jnp.concatenate([v[1:], empty], axis=0)
        from_left = pltpu.roll(left[it], lax.rem(LANES - x, LANES), 1)
        from_right = pltpu.roll(right[it], LANES - 1 - x, 1)
        beside = beside + jnp.where(lane == 0, from_left, pltpu.roll(v, 1, 1))
        beside = beside + jnp.where(lane == LANES - 1, from_right, pltpu.roll(v, LANES - 1, 1))
        return v, (6.0 + diag[x]) * v - beside

    sums = ((sum_a, "gz", gz, 4), (sum_b, "gx", gx, 4), (sum_c, "gy", gy, 8))

    def start_sum(it, stage, value):
        buffer, axis, me, count = sums[stage]
        buffer[it, me] = value
        for peer in others(axis, me, count):
            pltpu.make_async_remote_copy(
                buffer.at[it, me], buffer.at[it, me], sum_send.at[it, stage], sum_recv.at[it, stage],
                device_id=peer, device_id_type=MESH,
            ).start()

    def end_sum(it, stage):
        buffer, _, _, count = sums[stage]
        some = buffer.at[it, pl.ds(0, count - 1)]
        pltpu.make_async_copy(some, some, sum_recv.at[it, stage]).wait()
        total = buffer[it, 0]
        for k in range(1, count):
            total = total + buffer[it, k]
        return total

    def totals(it):
        total = end_sum(it, 2)
        whole = [jnp.sum(total[k], keepdims=True) for k in range(2)]
        return [jnp.broadcast_to(t, (8, LANES)) for t in whole]

    def folded(v):
        return jnp.sum(tiled(v), axis=0)

    def many(body):
        def some(i, carry):
            for j in range(UNROLL):
                carry = body(i * UNROLL + j, carry)
            return carry

        return some

    def rows_of(c, body, carry):
        begin = c * (CHUNK // UNROLL)
        return lax.fori_loop(begin, begin + CHUNK // UNROLL, many(body), carry)

    zero = jnp.zeros((8, LANES), f32)

    def first_precond(c, carry):
        some = res.at[pl.ds(pl.multiple_of(c * CHUNK, CHUNK), CHUNK)]
        pltpu.make_async_copy(some, some, col_sem.at[0, c]).wait()
        apply_blocks(res, u0, 0, c)
        return carry

    lax.fori_loop(0, STEPS, first_precond, 0)
    start_halo(u0, 0)
    for c in range(STEPS // 2, STEPS):
        send_columns(1, diagonal, diag, c)
    wait_halo(u0, 0)

    def first_image(c, carry):
        some = diag.at[pl.ds(pl.multiple_of(c * CHUNK, CHUNK), CHUNK)]
        pltpu.make_async_copy(some, some, col_sem.at[1, c]).wait()

        def body(x, carry):
            rz, wz = carry
            u, w = stencil(u0, 0, x)
            w0[x] = w
            return rz + folded(res[x] * u), wz + folded(w * u)

        return rows_of(c, body, carry)

    rz, wz = lax.fori_loop(0, STEPS, first_image, (zero, zero))

    def blocks_beside_sum(it, source, target):
        def body(c, carry):
            apply_blocks(source, target, it + 1, c)
            for stage in range(2):

                @pl.when(c == 2 * stage)
                def _():
                    start_sum(it, stage + 1, end_sum(it, stage))

            return carry

        lax.fori_loop(0, STEPS, body, 0)

    start_sum(0, 0, jnp.stack([rz, wz]))
    blocks_beside_sum(0, w0, m0)
    start_halo(m0, 1)
    rz0, wz0 = totals(0)
    alpha0 = rz0 / wz0
    wait_halo(m0, 1)

    def second(x, carry):
        rz, wz = carry
        m, n = stencil(m0, 1, x)
        n0[x] = n
        w = tiled(w0[x])
        r = tiled(res[x]) - alpha0 * w
        u = tiled(u0[x + 1]) - alpha0 * tiled(m)
        w = w - alpha0 * tiled(n)
        w1[x] = flat(w)
        return rz + jnp.sum(r * u, axis=0), wz + jnp.sum(w * u, axis=0)

    rz, wz = lax.fori_loop(0, ROWS // UNROLL, many(second), (zero, zero))
    start_sum(1, 0, jnp.stack([rz, wz]))
    blocks_beside_sum(1, w1, m1)
    start_halo(m1, 2)
    rz1, wz1 = totals(1)
    beta1 = rz1 / rz0
    alpha1 = rz1 / (wz1 - beta1 * rz1 / alpha0)
    wait_halo(m1, 2)

    def third(x, carry):
        rz, wz = carry
        m, n = stencil(m1, 2, x)
        first_w, second_w = tiled(w0[x]), tiled(w1[x])
        r = tiled(res[x]) - alpha0 * first_w - alpha1 * (second_w + beta1 * first_w)
        second_m = tiled(m0[x + 1])
        u = tiled(u0[x + 1]) - alpha0 * second_m - alpha1 * (tiled(m) + beta1 * second_m)
        w = second_w - alpha1 * (tiled(n) + beta1 * tiled(n0[x]))
        return rz + jnp.sum(r * u, axis=0), wz + jnp.sum(w * u, axis=0)

    rz, wz = lax.fori_loop(0, ROWS // UNROLL, many(third), (zero, zero))
    start_sum(2, 0, jnp.stack([rz, wz]))
    start_sum(2, 1, end_sum(2, 0))
    start_sum(2, 2, end_sum(2, 1))
    rz2, wz2 = totals(2)
    beta2 = rz2 / rz1
    alpha2 = rz2 / (wz2 - beta2 * rz2 / alpha1)

    by_u = alpha0 + alpha1 * (1.0 + beta1) + alpha2 * (1.0 + beta2 * (1.0 + beta1))
    by_m = -alpha1 * alpha0 - alpha2 * (alpha0 + alpha1 * beta1 + beta2 * alpha0)
    by_n = -alpha2 * alpha1

    def joined(u, m, n):
        return flat(by_u * tiled(u) + by_m * tiled(m) + by_n * tiled(n))

    def last_rows(x, carry):
        fin[x] = joined(u0[x], m0[x], m1[x])
        return carry

    lax.fori_loop(0, (ROWS + 2) // 6, lambda i, k: [last_rows(6 * i + j, k) for j in range(6)][0], 0)
    from_left, from_right = joined(left[0], left[1], left[2]), joined(right[0], right[1], right[2])
    sides[...] = jnp.where(lane < ROWS, from_left, pltpu.roll(from_right, ROWS, 1))

    mine = pl.ds(pl.multiple_of(part * ROWS, ROWS), ROWS)
    inner = fin.at[pl.ds(1, ROWS)]

    def give(k, source, target, recv):
        pltpu.make_async_remote_copy(
            source, target, out_send, recv, device_id={"gz": k}, device_id_type=MESH
        ).start()

    def keep(source, target, recv):
        pltpu.make_async_copy(source, target, recv).start()

    for j in range(1, 4):
        k = lax.rem(gz + j, 4)
        near = pl.ds(pl.multiple_of(k * SLAB, SLAB), SLAB)
        give(k, sides.at[near], out_sides.at[part], sides_recv)
        for end, here in enumerate((part == 0, part == 3)):
            row = end * (ROWS + 1)
            pl.when(here)(functools.partial(give, k, fin.at[row, near], out_ends.at[end], ends_recv))

        @pl.when(k > 0)
        def _():
            give(k, inner.at[:, k * SLAB - 1, :], out_sol.at[0, mine, :], out_recv)

        @pl.when(k < 3)
        def _():
            give(k, inner.at[:, k * SLAB + SLAB, :], out_sol.at[SLAB + 1, mine, :], out_recv)

    def send_back(d, carry):
        for j in range(1, 4):
            k = lax.rem(gz + j, 4)
            give(k, inner.at[:, k * SLAB + d, :], out_sol.at[d + 1, mine, :], out_recv)
        return carry

    lax.fori_loop(0, SLAB, send_back, 0)

    near = pl.ds(base, SLAB)
    keep(sides.at[near], out_sides.at[part], sides_recv)
    for end, here in enumerate((part == 0, part == 3)):
        row = end * (ROWS + 1)
        pl.when(here)(functools.partial(keep, fin.at[row, near], out_ends.at[end], ends_recv))

    def keep_own(d, carry):
        keep(inner.at[:, base + d, :], out_sol.at[d + 1, mine, :], out_recv)
        return carry

    lax.fori_loop(0, SLAB, keep_own, 0)
    for outside, plane, depth in ((gz == 0, 0, base - 1), (gz == 3, SLAB + 1, base + SLAB)):

        @pl.when(jnp.logical_not(outside))
        def _():
            keep(inner.at[:, depth, :], out_sol.at[plane, mine, :], out_recv)

        @pl.when(outside)
        def _():
            for k in range(4):
                keep(blank, out_sol.at[plane, pl.ds(k * ROWS, ROWS), :], out_recv)

    some = res.at[pl.ds(0, 3 * SLAB)]
    for array in range(2):
        pltpu.make_async_copy(some, some, in_send.at[array]).wait()
    for it, array in enumerate((u0, m0, m1)):
        for sends, _, copy in halo_copies(array, it):
            pl.when(sends)(copy.wait_send)
        for stage, (buffer, _, _, count) in enumerate(sums):
            group = buffer.at[it, pl.ds(0, count - 1)]
            pltpu.make_async_copy(group, group, sum_send.at[it, stage]).wait()
    for target, recv in ((out_sides, sides_recv), (out_ends, ends_recv), (out_sol, out_recv)):
        pltpu.make_async_copy(target, target, recv).wait()
    pltpu.make_async_copy(some, some, out_send).wait()
    pltpu.make_async_copy(sides.at[pl.ds(0, 3 * SLAB)], sides.at[pl.ds(0, 3 * SLAB)], out_send).wait()
    for _ in range(4):
        pltpu.make_async_copy(blank, blank, out_send).wait()

    @pl.when(jnp.logical_or(gz == 0, gz == 3))
    def _():
        pltpu.make_async_copy(blank, blank, out_send).wait()

    @pl.when(jnp.logical_or(part == 0, part == 3))
    def _():
        some_rows = blank.at[pl.ds(0, 3 * SLAB)]
        pltpu.make_async_copy(some_rows, some_rows, out_send).wait()


def residual_kernel(
    right_side, diagonal, inner, sides, ends, out_sol, out_res,
    sol, rhs, diag, res, side, end, turned, load, store,
):
    groups = SLAB // GROUP
    own = [pl.ds(g * GROUP, GROUP) for g in range(groups)]
    copies = [
        pltpu.make_async_copy(sides, side, load.at[2 * groups]),
        pltpu.make_async_copy(ends, end, load.at[2 * groups + 1]),
    ]
    planes, others = [], []
    for g in range(groups):
        begin = g * GROUP + (2 if g else 0)
        some = pl.ds(begin, GROUP + (0 if g else 2))
        planes.append(pltpu.make_async_copy(inner.at[some], sol.at[some], load.at[g]))
        others.append(
            [
                pltpu.make_async_copy(right_side.at[own[g]], rhs.at[own[g]], load.at[groups + g]),
                pltpu.make_async_copy(diagonal.at[own[g]], diag.at[own[g]], load.at[2 * groups + 2 + g]),
            ]
        )
    for copy in copies + [planes[0]] + others[0]:
        copy.start()
    for g in range(1, groups):
        for copy in [planes[g]] + others[g]:
            copy.start()
    for copy in copies:
        copy.wait()
    turned[...] = jnp.concatenate([side[...].reshape(DEEP, LANES), jnp.zeros((DEEP, LANES), f32)], axis=0).T
    lane = lax.broadcasted_iota(jnp.int32, (ROWS, LANES), 1)

    def plane(d, carry):
        for t in range(4):
            begin = t * ROWS
            rows = pl.ds(begin, ROWS)
            v = sol[d + 1, rows, :]
            beside = sol[d, rows, :] + sol[d + 2, rows, :]
            before = end[0, pl.ds(d, 1), :] if t == 0 else sol[d + 1, pl.ds(begin - 1, 1), :]
            after = end[1, pl.ds(d, 1), :] if t == 3 else sol[d + 1, pl.ds(begin + ROWS, 1), :]
            beside = beside + jnp.concatenate([before, v[:-1]], axis=0)
            beside = beside + jnp.concatenate([v[1:], after], axis=0)
            spot = t * SLAB + d
            from_left = pltpu.roll(turned[pl.ds(0, ROWS), :], lax.rem(LANES - spot, LANES), 1)
            from_right = pltpu.roll(turned[pl.ds(ROWS, ROWS), :], LANES - 1 - spot, 1)
            beside = beside + jnp.where(lane == 0, from_left, pltpu.roll(v, 1, 1))
            beside = beside + jnp.where(lane == LANES - 1, from_right, pltpu.roll(v, LANES - 1, 1))
            res[d, rows, :] = rhs[d, rows, :] - ((6.0 + diag[d, rows, :]) * v - beside)
        return carry

    stores = []
    for g in range(groups):
        for copy in [planes[g]] + others[g]:
            copy.wait()
        lax.fori_loop(g * GROUP, (g + 1) * GROUP, plane, 0)
        stores += [
            pltpu.make_async_copy(res.at[own[g]], out_res.at[own[g]], store.at[0, g]),
            pltpu.make_async_copy(
                sol.at[pl.ds(g * GROUP + 1, GROUP)], out_sol.at[own[g]], store.at[1, g]
            ),
        ]
        for copy in stores[-2:]:
            copy.start()
    for copy in stores:
        copy.wait()


def per_device(right_side, diagonal, regime, inverses):
    shape = jax.ShapeDtypeStruct(right_side.shape, f32)
    field = pltpu.VMEM((ROWS, DEEP, LANES), f32)
    padded = pltpu.VMEM((ROWS + 2, DEEP, LANES), f32)
    plane = (DEEP, LANES)
    anywhere = pl.BlockSpec(memory_space=pl.ANY)
    wide = (SLAB + 2,) + right_side.shape[1:]
    inner, sides, ends = pl.pallas_call(
        kernel,
        out_shape=(
            jax.ShapeDtypeStruct(wide, f32),
            jax.ShapeDtypeStruct((4, SLAB, LANES), f32),
            jax.ShapeDtypeStruct((2, SLAB, LANES), f32),
        ),
        in_specs=[anywhere] * 4,
        out_specs=[anywhere] * 3,
        scratch_shapes=[
            field, field, padded, padded, padded, field, field, field, padded,
            pltpu.VMEM((ROWS, LANES), jnp.int32),
            pltpu.VMEM((NREG * DEEP, DEEP), f32),
            pltpu.VMEM((NREG * DEEP, 4 * DEEP), bf16),
            pltpu.VMEM((3, 2) + plane, f32),
            pltpu.VMEM((3,) + plane, f32),
            pltpu.VMEM((3,) + plane, f32),
            pltpu.VMEM(plane, f32),
            pltpu.VMEM(plane, f32),
            pltpu.VMEM((3, 4, 2, 8, LANES), f32),
            pltpu.VMEM((3, 4, 2, 8, LANES), f32),
            pltpu.VMEM((3, 8, 2, 8, LANES), f32),
            pltpu.SemaphoreType.DMA((2, STEPS)),
            pltpu.SemaphoreType.DMA((2,)),
            pltpu.SemaphoreType.DMA((2,)),
            pltpu.SemaphoreType.DMA((3, 4)),
            pltpu.SemaphoreType.DMA((3, 4)),
            pltpu.SemaphoreType.DMA((3, 3)),
            pltpu.SemaphoreType.DMA((3, 3)),
            pltpu.SemaphoreType.DMA,
            pltpu.SemaphoreType.DMA,
            pltpu.SemaphoreType.DMA,
            pltpu.SemaphoreType.DMA,
        ],
        compiler_params=pltpu.CompilerParams(
            collective_id=0, has_side_effects=True, vmem_limit_bytes=60 * 2**20
        ),
    )(right_side, diagonal, regime, inverses.reshape(NREG * DEEP, DEEP))
    slab = pltpu.VMEM(right_side.shape, f32)
    groups = SLAB // GROUP
    return pl.pallas_call(
        residual_kernel,
        out_shape=(shape, shape),
        in_specs=[anywhere] * 5,
        out_specs=[anywhere] * 2,
        scratch_shapes=[
            pltpu.VMEM(wide, f32), slab, slab, slab,
            pltpu.VMEM((4, SLAB, LANES), f32),
            pltpu.VMEM((2, SLAB, LANES), f32),
            pltpu.VMEM((LANES, LANES), f32),
            pltpu.SemaphoreType.DMA((3 * groups + 2,)),
            pltpu.SemaphoreType.DMA((2, groups)),
        ],
        compiler_params=pltpu.CompilerParams(vmem_limit_bytes=60 * 2**20),
    )(right_side, diagonal, inner, sides, ends)


def solution(mesh):
    field = P("gz", "gx", "gy")
    return jax.shard_map(
        per_device,
        mesh=mesh,
        in_specs=(field, field, P("gx", "gy"), P()),
        out_specs=(field, field),
        check_vma=False,
    )
```

```python
import functools

import jax
import jax.numpy as jnp
from jax import lax
from jax.experimental import pallas as pl
from jax.experimental.pallas import tpu as pltpu
from jax.sharding import PartitionSpec as P

f32 = jnp.float32
bf16 = jnp.bfloat16
MESH = pl.DeviceIdType.MESH
NREG = 8
ROWS = 64
DEEP = 64
SLAB = 16
LANES = 128
CHUNK = 16
STEPS = ROWS // CHUNK
DEVICES = 128
ORDER = (0, 3, 1, 2)
UNROLL = 8
GROUP = 4


def halves(v):
    high = v.astype(bf16)
    return high, (v - high.astype(f32)).astype(bf16)


def tiled(v):
    return v.reshape(DEEP // 8, 8, LANES)


def flat(v):
    return v.reshape(DEEP, LANES)


def kernel(
    right_side, diagonal, regime, blocks,
    out_sol, out_sides, out_ends,
    res, diag, u0, m0, m1, w0, n0, n1, w1, fin,
    reg, inv, stack, edge, left, right, border, sides, blank, sums,
    col_sem, in_send, small_sem, halo_recv, halo_send, sum_recv, sum_send, out_recv, sides_recv, ends_recv, out_send,
):
    gx, gy, gz = lax.axis_index("gx"), lax.axis_index("gy"), lax.axis_index("gz")
    odd = lax.rem(gx, 2)
    part = gz + odd * (3 - 2 * gz)
    stride = 1 - 2 * odd
    first, last = (3 - part) // 3, part // 3
    line = gx * 4 + part
    lower = {"gx": gx - first, "gz": gz - stride * (1 - first)}
    upper = {"gx": gx + last, "gz": gz + stride * (1 - last)}
    has_lower, has_upper = line > 0, line < 15
    has_left, has_right = gy > 0, gy < 7

    everyone = [
        {"gx": lax.rem(gx + a, 4), "gy": lax.rem(gy + b, 8), "gz": lax.rem(gz + c, 4)}
        for a in (2, 1, 3, 0) for b in (4, 3, 5, 2, 6, 1, 7, 0) for c in (2, 3, 1, 0)
    ][:-1]
    barrier = pltpu.get_barrier_semaphore()
    for peer in everyone:
        pl.semaphore_signal(barrier, inc=1, device_id=peer, device_id_type=MESH)

    small = [
        pltpu.make_async_copy(blocks, inv, small_sem.at[0]),
        pltpu.make_async_copy(
            regime.at[pl.ds(pl.multiple_of(part * ROWS, ROWS), ROWS), :], reg, small_sem.at[1]
        ),
    ]
    for copy in small:
        copy.start()
    base = pl.multiple_of(gz * SLAB, SLAB)

    def part_of(k):
        return k + odd * (3 - 2 * k)

    def send_columns(array, source, target, c):
        def body(d, carry):
            rows = pl.ds(c * CHUNK, CHUNK)
            for j in range(1, 4):
                k = lax.rem(gz + j, 4)
                begin = pl.multiple_of(part_of(k) * ROWS + c * CHUNK, CHUNK)
                pltpu.make_async_remote_copy(
                    source.at[d, pl.ds(begin, CHUNK), :],
                    target.at[rows, base + d, :],
                    in_send.at[array],
                    col_sem.at[array, c],
                    device_id={"gz": k},
                    device_id_type=MESH,
                ).start()
            begin = pl.multiple_of(part * ROWS + c * CHUNK, CHUNK)
            pltpu.make_async_copy(
                source.at[d, pl.ds(begin, CHUNK), :],
                target.at[rows, base + d, :],
                col_sem.at[array, c],
            ).start()
            return carry

        lax.fori_loop(0, SLAB, body, 0)

    pl.semaphore_wait(barrier, DEVICES - 1)
    for c in ORDER:
        send_columns(0, right_side, res, c)
    for c in ORDER[:2]:
        send_columns(1, diagonal, diag, c)

    nothing = jnp.zeros((DEEP, LANES), f32)
    blank[...] = nothing
    for array in (u0, m0, m1):

        @pl.when(line == 0)
        def _():
            array[0] = nothing

        @pl.when(line == 15)
        def _():
            array[ROWS + 1] = nothing

    for it in range(3):

        @pl.when(gy == 0)
        def _():
            left[it] = nothing

        @pl.when(gy == 7)
        def _():
            right[it] = nothing

        edge[it] = nothing

    for copy in small:
        copy.wait()
    high, low = halves(inv[...])
    stack[...] = jnp.concatenate([high, high, low, low], axis=1)

    lane = lax.broadcasted_iota(jnp.int32, (DEEP, LANES), 1)

    def apply_blocks(source, target, it, c):
        ends = edge[it]
        for h in range(CHUNK // 2):
            x = c * CHUNK + 2 * h
            both = jnp.concatenate([source[x], source[x + 1]], axis=1)
            high, low = halves(both)
            out = jnp.dot(
                stack[...],
                jnp.concatenate([high, low, high, low], axis=0),
                preferred_element_type=f32,
            )
            kind = jnp.concatenate([reg[pl.ds(x, 1), :], reg[pl.ds(x + 1, 1), :]], axis=1)
            kind = jnp.broadcast_to(kind, (DEEP, 2 * LANES))
            some = [out[k * DEEP : (k + 1) * DEEP] for k in range(NREG)]
            for bit in range(3):
                chosen = (kind & (1 << bit)) != 0
                some = [jnp.where(chosen, some[i + 1], some[i]) for i in range(0, len(some), 2)]
            for j in range(2):
                z = some[0][:, j * LANES : (j + 1) * LANES]
                target[x + j + 1] = z
                turned = pltpu.roll(z, 2 * (x + j) + 1, 1)
                ends = jnp.where((lane == 2 * (x + j)) | (lane == 2 * (x + j) + 1), turned, ends)
        edge[it] = ends

    def halo_copies(array, it):
        def copy(k, source, target, device):
            return pltpu.make_async_remote_copy(
                source, target, halo_send.at[it, k], halo_recv.at[it, k],
                device_id=device, device_id_type=MESH,
            )

        copy = functools.partial(functools.partial, copy)
        return (
            (has_lower, has_upper, copy(0, array.at[1], array.at[ROWS + 1], lower)),
            (has_upper, has_lower, copy(1, array.at[ROWS], array.at[0], upper)),
            (has_left, has_right, copy(2, edge.at[it], right.at[it], {"gy": gy - 1})),
            (has_right, has_left, copy(3, edge.at[it], left.at[it], {"gy": gy + 1})),
        )

    def start_halo(array, it, which):
        for sends, _, copy in halo_copies(array, it)[which]:
            pl.when(sends)(lambda: copy().start())

    def wait_halo(array, it, which):
        for _, receives, copy in halo_copies(array, it)[which]:
            pl.when(receives)(lambda: copy().wait_recv())

    along_rows, along_lanes = slice(0, 2), slice(2, 4)
    even = lax.rem(lane, 2) == 0
    outer = (lane == 0) | (lane == LANES - 1)

    def set_border(it):
        border[...] = jnp.where(even, left[it], pltpu.roll(right[it], LANES - 2, 1))

    def beyond(x):
        turned = pltpu.roll(border[...], lax.rem(LANES - 2 * x, LANES), 1)
        return jnp.where(outer, turned, 0.0)

    def stencil(array, x):
        v = array[x + 1]
        beside = array[x] + array[x + 2]
        empty = jnp.zeros((1, LANES), f32)
        beside = beside + jnp.concatenate([empty, v[:-1]], axis=0)
        beside = beside + jnp.concatenate([v[1:], empty], axis=0)
        beside = beside + jnp.where(lane == 0, 0.0, pltpu.roll(v, 1, 1))
        beside = beside + jnp.where(lane == LANES - 1, 0.0, pltpu.roll(v, LANES - 1, 1))
        return v, (6.0 + diag[x]) * v - beside

    me = (gx * 8 + gy) * 4 + gz
    lower_half = lax.broadcasted_iota(jnp.int32, (1, LANES), 1) < LANES // 2

    def start_sum(it, rz, wz):
        rows = [jnp.sum(v, axis=0, keepdims=True) for v in (rz, wz)]
        rows = [row + pltpu.roll(row, LANES // 2, 1) for row in rows]
        sums[it, pl.ds(me, 1), :] = jnp.where(lower_half, rows[0], rows[1])
        for peer in everyone:
            pltpu.make_async_remote_copy(
                sums.at[it, me], sums.at[it, me], sum_send.at[it], sum_recv.at[it],
                device_id=peer, device_id_type=MESH,
            ).start()

    def totals(it):
        some = sums.at[it, pl.ds(0, DEVICES - 1)]
        pltpu.make_async_copy(some, some, sum_recv.at[it]).wait()
        total = jnp.sum(sums[it], axis=0, keepdims=True)
        rz = jnp.sum(jnp.where(lower_half, total, 0.0), keepdims=True)
        wz = jnp.sum(jnp.where(lower_half, 0.0, total), keepdims=True)
        return [jnp.broadcast_to(v, (8, LANES)) for v in (rz, wz)]

    def folded(v):
        return jnp.sum(tiled(v), axis=0)

    def many(body):
        def some(i, carry):
            for j in range(UNROLL):
                carry = body(i * UNROLL + j, carry)
            return carry

        return some

    def rows_of(c, body, carry):
        begin = c * (CHUNK // UNROLL)
        return lax.fori_loop(begin, begin + CHUNK // UNROLL, many(body), carry)

    zero = jnp.zeros((8, LANES), f32)

    def ordered(i):
        return 3 * i - (i // 2) * (2 * i + 1)

    def blocks_pass(it, source, target, before):
        def body(i, carry):
            c = ordered(i)
            before(c)
            apply_blocks(source, target, it, c)

            @pl.when(i == 1)
            def _():
                start_halo(target, it, along_rows)

            return carry

        lax.fori_loop(0, STEPS, body, 0)
        start_halo(target, it, along_lanes)

    def arrived(array, target):
        def wait(c):
            some = target.at[pl.ds(pl.multiple_of(c * CHUNK, CHUNK), CHUNK)]
            pltpu.make_async_copy(some, some, col_sem.at[array, c]).wait()

        return wait

    blocks_pass(0, res, u0, arrived(0, res))
    for c in ORDER[2:]:
        send_columns(1, diagonal, diag, c)
    wait_halo(u0, 0, along_rows)
    wait_halo(u0, 0, along_lanes)
    set_border(0)

    def first_image(i, carry):
        c = ordered(i)
        arrived(1, diag)(c)

        def body(x, carry):
            rz, wz = carry
            u, w = stencil(u0, x)
            w = w - beyond(x)
            w0[x] = w
            return rz + folded(res[x] * u), wz + folded(w * u)

        return rows_of(c, body, carry)

    start_sum(0, *lax.fori_loop(0, STEPS, first_image, (zero, zero)))

    def image_pass(it, array, target):
        def body(x, carry):
            _, target[x] = stencil(array, x)
            return carry

        lax.fori_loop(CHUNK // UNROLL, (ROWS - CHUNK) // UNROLL, many(body), 0)
        wait_halo(array, it, along_rows)
        rows_of(0, body, 0)
        rows_of(STEPS - 1, body, 0)

    blocks_pass(1, w0, m0, lambda c: None)
    image_pass(1, m0, n0)
    wait_halo(m0, 1, along_lanes)
    set_border(1)
    rz0, wz0 = totals(0)
    alpha0 = rz0 / wz0

    def second(x, carry):
        rz, wz = carry
        n = n0[x] - beyond(x)
        n0[x] = n
        w = tiled(w0[x])
        r = tiled(res[x]) - alpha0 * w
        u = tiled(u0[x + 1]) - alpha0 * tiled(m0[x + 1])
        w = w - alpha0 * tiled(n)
        w1[x] = flat(w)
        return rz + jnp.sum(r * u, axis=0), wz + jnp.sum(w * u, axis=0)

    start_sum(1, *lax.fori_loop(0, ROWS // UNROLL, many(second), (zero, zero)))
    blocks_pass(2, w1, m1, lambda c: None)
    image_pass(2, m1, n1)
    wait_halo(m1, 2, along_lanes)
    set_border(2)
    rz1, wz1 = totals(1)
    beta1 = rz1 / rz0
    alpha1 = rz1 / (wz1 - beta1 * rz1 / alpha0)

    def third(x, carry):
        rz, wz = carry
        n = n1[x] - beyond(x)
        first_w, second_w = tiled(w0[x]), tiled(w1[x])
        r = tiled(res[x]) - alpha0 * first_w - alpha1 * (second_w + beta1 * first_w)
        second_m = tiled(m0[x + 1])
        u = tiled(u0[x + 1]) - alpha0 * second_m - alpha1 * (tiled(m1[x + 1]) + beta1 * second_m)
        w = second_w - alpha1 * (tiled(n) + beta1 * tiled(n0[x]))
        return rz + jnp.sum(r * u, axis=0), wz + jnp.sum(w * u, axis=0)

    start_sum(2, *lax.fori_loop(0, ROWS // UNROLL, many(third), (zero, zero)))
    rz2, wz2 = totals(2)
    beta2 = rz2 / rz1
    alpha2 = rz2 / (wz2 - beta2 * rz2 / alpha1)

    by_u = alpha0 + alpha1 * (1.0 + beta1) + alpha2 * (1.0 + beta2 * (1.0 + beta1))
    by_m = -alpha1 * alpha0 - alpha2 * (alpha0 + alpha1 * beta1 + beta2 * alpha0)
    by_n = -alpha2 * alpha1

    def joined(u, m, n):
        return flat(by_u * tiled(u) + by_m * tiled(m) + by_n * tiled(n))

    def last_rows(x, carry):
        fin[x] = joined(u0[x], m0[x], m1[x])
        return carry

    lax.fori_loop(0, (ROWS + 2) // 6, lambda i, k: [last_rows(6 * i + j, k) for j in range(6)][0], 0)
    sides[...] = joined(*[jnp.where(even, left[it], right[it]) for it in range(3)])

    mine = pl.ds(pl.multiple_of(part * ROWS, ROWS), ROWS)
    inner = fin.at[pl.ds(1, ROWS)]

    def give(k, source, target, recv):
        pltpu.make_async_remote_copy(
            source, target, out_send, recv, device_id={"gz": k}, device_id_type=MESH
        ).start()

    def keep(source, target, recv):
        pltpu.make_async_copy(source, target, recv).start()

    for j in range(1, 4):
        k = lax.rem(gz + j, 4)
        near = pl.ds(pl.multiple_of(k * SLAB, SLAB), SLAB)
        give(k, sides.at[near], out_sides.at[part], sides_recv)
        for end, here in enumerate((part == 0, part == 3)):
            row = end * (ROWS + 1)
            pl.when(here)(functools.partial(give, k, fin.at[row, near], out_ends.at[end], ends_recv))

        @pl.when(k > 0)
        def _():
            give(k, inner.at[:, k * SLAB - 1, :], out_sol.at[0, mine, :], out_recv)

        @pl.when(k < 3)
        def _():
            give(k, inner.at[:, k * SLAB + SLAB, :], out_sol.at[SLAB + 1, mine, :], out_recv)

    def send_back(d, carry):
        for j in range(1, 4):
            k = lax.rem(gz + j, 4)
            give(k, inner.at[:, k * SLAB + d, :], out_sol.at[d + 1, mine, :], out_recv)
        return carry

    lax.fori_loop(0, SLAB, send_back, 0)

    near = pl.ds(base, SLAB)
    keep(sides.at[near], out_sides.at[part], sides_recv)
    for end, here in enumerate((part == 0, part == 3)):
        row = end * (ROWS + 1)
        pl.when(here)(functools.partial(keep, fin.at[row, near], out_ends.at[end], ends_recv))

    def keep_own(d, carry):
        keep(inner.at[:, base + d, :], out_sol.at[d + 1, mine, :], out_recv)
        return carry

    lax.fori_loop(0, SLAB, keep_own, 0)
    for outside, plane, depth in ((gz == 0, 0, base - 1), (gz == 3, SLAB + 1, base + SLAB)):

        @pl.when(jnp.logical_not(outside))
        def _():
            keep(inner.at[:, depth, :], out_sol.at[plane, mine, :], out_recv)

        @pl.when(outside)
        def _():
            for k in range(4):
                keep(blank, out_sol.at[plane, pl.ds(k * ROWS, ROWS), :], out_recv)

    some = res.at[pl.ds(0, 3 * SLAB)]
    for array in range(2):
        pltpu.make_async_copy(some, some, in_send.at[array]).wait()
    for it, array in enumerate((u0, m0, m1)):
        for sends, _, copy in halo_copies(array, it):
            pl.when(sends)(lambda: copy().wait_send())
        group = sums.at[it, pl.ds(0, DEVICES - 1)]
        pltpu.make_async_copy(group, group, sum_send.at[it]).wait()
    for target, recv in ((out_sides, sides_recv), (out_ends, ends_recv), (out_sol, out_recv)):
        pltpu.make_async_copy(target, target, recv).wait()
    pltpu.make_async_copy(some, some, out_send).wait()
    pltpu.make_async_copy(sides.at[pl.ds(0, 3 * SLAB)], sides.at[pl.ds(0, 3 * SLAB)], out_send).wait()
    for _ in range(4):
        pltpu.make_async_copy(blank, blank, out_send).wait()

    @pl.when(jnp.logical_or(gz == 0, gz == 3))
    def _():
        pltpu.make_async_copy(blank, blank, out_send).wait()

    @pl.when(jnp.logical_or(part == 0, part == 3))
    def _():
        some_rows = blank.at[pl.ds(0, 3 * SLAB)]
        pltpu.make_async_copy(some_rows, some_rows, out_send).wait()


def residual_kernel(
    right_side, diagonal, inner, sides, ends, out_sol, out_res,
    sol, rhs, diag, res, side, end, whole, turned, load, store,
):
    groups = SLAB // GROUP
    own = [pl.ds(g * GROUP, GROUP) for g in range(groups)]
    copies = [
        pltpu.make_async_copy(sides, side, load.at[2 * groups]),
        pltpu.make_async_copy(ends, end, load.at[2 * groups + 1]),
    ]
    planes, others = [], []
    for g in range(groups):
        begin = g * GROUP + (2 if g else 0)
        some = pl.ds(begin, GROUP + (0 if g else 2))
        planes.append(pltpu.make_async_copy(inner.at[some], sol.at[some], load.at[g]))
        others.append(
            [
                pltpu.make_async_copy(right_side.at[own[g]], rhs.at[own[g]], load.at[groups + g]),
                pltpu.make_async_copy(diagonal.at[own[g]], diag.at[own[g]], load.at[2 * groups + 2 + g]),
            ]
        )
    for copy in copies + [planes[0]] + others[0]:
        copy.start()
    for g in range(1, groups):
        for copy in [planes[g]] + others[g]:
            copy.start()
    for copy in copies:
        copy.wait()
    whole[...] = jnp.concatenate([side[...].reshape(DEEP, LANES), jnp.zeros((DEEP, LANES), f32)], axis=0).T
    for k in range(2):
        turned[k] = whole[pl.ds(k, ROWS, stride=2), :]
    lane = lax.broadcasted_iota(jnp.int32, (ROWS, LANES), 1)

    def plane(d, carry):
        for t in range(4):
            begin = t * ROWS
            rows = pl.ds(begin, ROWS)
            v = sol[d + 1, rows, :]
            beside = sol[d, rows, :] + sol[d + 2, rows, :]
            before = end[0, pl.ds(d, 1), :] if t == 0 else sol[d + 1, pl.ds(begin - 1, 1), :]
            after = end[1, pl.ds(d, 1), :] if t == 3 else sol[d + 1, pl.ds(begin + ROWS, 1), :]
            beside = beside + jnp.concatenate([before, v[:-1]], axis=0)
            beside = beside + jnp.concatenate([v[1:], after], axis=0)
            spot = t * SLAB + d
            from_left = pltpu.roll(turned[0], lax.rem(LANES - spot, LANES), 1)
            from_right = pltpu.roll(turned[1], LANES - 1 - spot, 1)
            beside = beside + jnp.where(lane == 0, from_left, pltpu.roll(v, 1, 1))
            beside = beside + jnp.where(lane == LANES - 1, from_right, pltpu.roll(v, LANES - 1, 1))
            res[d, rows, :] = rhs[d, rows, :] - ((6.0 + diag[d, rows, :]) * v - beside)
        return carry

    stores = []
    for g in range(groups):
        for copy in [planes[g]] + others[g]:
            copy.wait()
        lax.fori_loop(g * GROUP, (g + 1) * GROUP, plane, 0)
        stores += [
            pltpu.make_async_copy(res.at[own[g]], out_res.at[own[g]], store.at[0, g]),
            pltpu.make_async_copy(
                sol.at[pl.ds(g * GROUP + 1, GROUP)], out_sol.at[own[g]], store.at[1, g]
            ),
        ]
        for copy in stores[-2:]:
            copy.start()
    for copy in stores:
        copy.wait()


def per_device(right_side, diagonal, regime, inverses):
    shape = jax.ShapeDtypeStruct(right_side.shape, f32)
    field = pltpu.VMEM((ROWS, DEEP, LANES), f32)
    padded = pltpu.VMEM((ROWS + 2, DEEP, LANES), f32)
    plane = (DEEP, LANES)
    anywhere = pl.BlockSpec(memory_space=pl.ANY)
    wide = (SLAB + 2,) + right_side.shape[1:]
    inner, sides, ends = pl.pallas_call(
        kernel,
        out_shape=(
            jax.ShapeDtypeStruct(wide, f32),
            jax.ShapeDtypeStruct((4, SLAB, LANES), f32),
            jax.ShapeDtypeStruct((2, SLAB, LANES), f32),
        ),
        in_specs=[anywhere] * 4,
        out_specs=[anywhere] * 3,
        scratch_shapes=[
            field, field, padded, padded, padded, field, field, field, field, padded,
            pltpu.VMEM((ROWS, LANES), jnp.int32),
            pltpu.VMEM((NREG * DEEP, DEEP), f32),
            pltpu.VMEM((NREG * DEEP, 4 * DEEP), bf16),
            pltpu.VMEM((3,) + plane, f32),
            pltpu.VMEM((3,) + plane, f32),
            pltpu.VMEM((3,) + plane, f32),
            pltpu.VMEM(plane, f32),
            pltpu.VMEM(plane, f32),
            pltpu.VMEM(plane, f32),
            pltpu.VMEM((3, DEVICES, LANES), f32),
            pltpu.SemaphoreType.DMA((2, STEPS)),
            pltpu.SemaphoreType.DMA((2,)),
            pltpu.SemaphoreType.DMA((2,)),
            pltpu.SemaphoreType.DMA((3, 4)),
            pltpu.SemaphoreType.DMA((3, 4)),
            pltpu.SemaphoreType.DMA((3,)),
            pltpu.SemaphoreType.DMA((3,)),
            pltpu.SemaphoreType.DMA,
            pltpu.SemaphoreType.DMA,
            pltpu.SemaphoreType.DMA,
            pltpu.SemaphoreType.DMA,
        ],
        compiler_params=pltpu.CompilerParams(
            collective_id=0, has_side_effects=True, vmem_limit_bytes=60 * 2**20
        ),
    )(right_side, diagonal, regime, inverses.reshape(NREG * DEEP, DEEP))
    slab = pltpu.VMEM(right_side.shape, f32)
    groups = SLAB // GROUP
    return pl.pallas_call(
        residual_kernel,
        out_shape=(shape, shape),
        in_specs=[anywhere] * 5,
        out_specs=[anywhere] * 2,
        scratch_shapes=[
            pltpu.VMEM(wide, f32), slab, slab, slab,
            pltpu.VMEM((4, SLAB, LANES), f32),
            pltpu.VMEM((2, SLAB, LANES), f32),
            pltpu.VMEM((LANES, LANES), f32),
            pltpu.VMEM((2, ROWS, LANES), f32),
            pltpu.SemaphoreType.DMA((3 * groups + 2,)),
            pltpu.SemaphoreType.DMA((2, groups)),
        ],
        compiler_params=pltpu.CompilerParams(vmem_limit_bytes=60 * 2**20),
    )(right_side, diagonal, inner, sides, ends)


def solution(mesh):
    field = P("gz", "gx", "gy")
    return jax.shard_map(
        per_device,
        mesh=mesh,
        in_specs=(field, field, P("gx", "gy"), P()),
        out_specs=(field, field),
        check_vma=False,
    )
```

```python
import functools

import jax
import jax.numpy as jnp
from jax import lax
from jax.experimental import pallas as pl
from jax.experimental.pallas import tpu as pltpu
from jax.sharding import PartitionSpec as P

f32 = jnp.float32
bf16 = jnp.bfloat16
MESH = pl.DeviceIdType.MESH
NREG = 8
ROWS = 64
DEEP = 64
SLAB = 16
LANES = 128
CHUNK = 16
STEPS = ROWS // CHUNK
DEVICES = 128
ORDER = (0, 3, 1, 2)
UNROLL = 16
GROUP = 4


def halves(v):
    high = v.astype(bf16)
    return high, (v - high.astype(f32)).astype(bf16)


def tiled(v):
    return v.reshape(DEEP // 8, 8, LANES)


def flat(v):
    return v.reshape(DEEP, LANES)


def kernel(
    right_side, diagonal, regime, blocks,
    out_sol, out_sides, out_ends,
    res, diag, u0, m0, m1, w0, n0, n1, w1, fin,
    reg, inv, stack, edge, left, right, border, sides, blank, sums,
    rounds, col_sem, in_send, small_sem, halo_recv, halo_send, sum_recv, sum_send, out_recv, sides_recv, ends_recv, out_send,
):
    gx, gy, gz = lax.axis_index("gx"), lax.axis_index("gy"), lax.axis_index("gz")
    odd = lax.rem(gx, 2)
    part = gz + odd * (3 - 2 * gz)
    stride = 1 - 2 * odd
    first, last = (3 - part) // 3, part // 3
    line = gx * 4 + part
    lower = {"gx": gx - first, "gz": gz - stride * (1 - first)}
    upper = {"gx": gx + last, "gz": gz + stride * (1 - last)}
    has_lower, has_upper = line > 0, line < 15
    has_left, has_right = gy > 0, gy < 7

    everyone = [
        {"gx": lax.rem(gx + a, 4), "gy": lax.rem(gy + b, 8), "gz": lax.rem(gz + c, 4)}
        for a in (2, 1, 3, 0) for b in (4, 3, 5, 2, 6, 1, 7, 0) for c in (2, 3, 1, 0)
    ][:-1]
    barrier = pltpu.get_barrier_semaphore()
    layer, side, slot, core = gy // 2, lax.rem(gy, 2), gz // 2, lax.rem(gz, 2)
    near_by = [{"gz": lax.rem(gz + j, 4)} for j in (1, 2, 3)]
    near_by += [{"gx": lax.rem(gx + j, 4)} for j in (1, 3)]
    near_by += [{"gy": lax.rem(gy + j, 8)} for j in (2, 6)]
    near_by += [{"gy": 2 * layer + 1 - side, "gz": 2 * (1 - slot) + core}]

    def tell(semaphore):
        for peer in near_by:
            pl.semaphore_signal(semaphore, inc=1, device_id=peer, device_id_type=MESH)

    def spread(k):
        tell(rounds.at[k])
        pl.semaphore_wait(rounds.at[k], len(near_by))

    tell(barrier)

    small = [
        pltpu.make_async_copy(blocks, inv, small_sem.at[0]),
        pltpu.make_async_copy(
            regime.at[pl.ds(pl.multiple_of(part * ROWS, ROWS), ROWS), :], reg, small_sem.at[1]
        ),
    ]
    for copy in small:
        copy.start()
    base = pl.multiple_of(gz * SLAB, SLAB)

    def part_of(k):
        return k + odd * (3 - 2 * k)

    def send_columns(array, source, target, c):
        def body(d, carry):
            rows = pl.ds(c * CHUNK, CHUNK)
            for j in range(1, 4):
                k = lax.rem(gz + j, 4)
                begin = pl.multiple_of(part_of(k) * ROWS + c * CHUNK, CHUNK)
                pltpu.make_async_remote_copy(
                    source.at[d, pl.ds(begin, CHUNK), :],
                    target.at[rows, base + d, :],
                    in_send.at[array],
                    col_sem.at[array, c],
                    device_id={"gz": k},
                    device_id_type=MESH,
                ).start()
            begin = pl.multiple_of(part * ROWS + c * CHUNK, CHUNK)
            pltpu.make_async_copy(
                source.at[d, pl.ds(begin, CHUNK), :],
                target.at[rows, base + d, :],
                col_sem.at[array, c],
            ).start()
            return carry

        lax.fori_loop(0, SLAB, body, 0)

    pl.semaphore_wait(barrier, len(near_by))
    for c in ORDER:
        send_columns(0, right_side, res, c)
    for c in ORDER[:2]:
        send_columns(1, diagonal, diag, c)

    nothing = jnp.zeros((DEEP, LANES), f32)
    blank[...] = nothing
    for array in (u0, m0, m1):

        @pl.when(line == 0)
        def _():
            array[0] = nothing

        @pl.when(line == 15)
        def _():
            array[ROWS + 1] = nothing

    for it in range(3):

        @pl.when(gy == 0)
        def _():
            left[it] = nothing

        @pl.when(gy == 7)
        def _():
            right[it] = nothing

        edge[it] = nothing

    for copy in small:
        copy.wait()
    high, low = halves(inv[...])
    stack[...] = jnp.concatenate([high, high, low, low], axis=1)

    lane = lax.broadcasted_iota(jnp.int32, (DEEP, LANES), 1)

    def apply_blocks(source, target, it, c):
        ends = edge[it]
        for h in range(CHUNK // 2):
            x = c * CHUNK + 2 * h
            both = jnp.concatenate([source[x], source[x + 1]], axis=1)
            high, low = halves(both)
            out = jnp.dot(
                stack[...],
                jnp.concatenate([high, low, high, low], axis=0),
                preferred_element_type=f32,
            )
            kind = jnp.concatenate([reg[pl.ds(x, 1), :], reg[pl.ds(x + 1, 1), :]], axis=1)
            kind = jnp.broadcast_to(kind, (DEEP, 2 * LANES))
            some = [out[k * DEEP : (k + 1) * DEEP] for k in range(NREG)]
            for bit in range(3):
                chosen = (kind & (1 << bit)) != 0
                some = [jnp.where(chosen, some[i + 1], some[i]) for i in range(0, len(some), 2)]
            for j in range(2):
                z = some[0][:, j * LANES : (j + 1) * LANES]
                target[x + j + 1] = z
                turned = pltpu.roll(z, 2 * (x + j) + 1, 1)
                ends = jnp.where((lane == 2 * (x + j)) | (lane == 2 * (x + j) + 1), turned, ends)
        edge[it] = ends

    def halo_copies(array, it):
        def copy(k, source, target, device):
            return pltpu.make_async_remote_copy(
                source, target, halo_send.at[it, k], halo_recv.at[it, k],
                device_id=device, device_id_type=MESH,
            )

        copy = functools.partial(functools.partial, copy)
        return (
            (has_lower, has_upper, copy(0, array.at[1], array.at[ROWS + 1], lower)),
            (has_upper, has_lower, copy(1, array.at[ROWS], array.at[0], upper)),
            (has_left, has_right, copy(2, edge.at[it], right.at[it], {"gy": gy - 1})),
            (has_right, has_left, copy(3, edge.at[it], left.at[it], {"gy": gy + 1})),
        )

    def start_halo(array, it, which):
        for sends, _, copy in halo_copies(array, it)[which]:
            pl.when(sends)(lambda: copy().start())

    def wait_halo(array, it, which):
        for _, receives, copy in halo_copies(array, it)[which]:
            pl.when(receives)(lambda: copy().wait_recv())

    along_rows, along_lanes = slice(0, 2), slice(2, 4)
    even = lax.rem(lane, 2) == 0
    outer = (lane == 0) | (lane == LANES - 1)

    def set_border(it):
        border[...] = jnp.where(even, left[it], pltpu.roll(right[it], LANES - 2, 1))

    def beyond(x):
        turned = pltpu.roll(border[...], lax.rem(LANES - 2 * x, LANES), 1)
        return jnp.where(outer, turned, 0.0)

    def stencil(array, x):
        v = array[x + 1]
        beside = array[x] + array[x + 2]
        empty = jnp.zeros((1, LANES), f32)
        beside = beside + jnp.concatenate([empty, v[:-1]], axis=0)
        beside = beside + jnp.concatenate([v[1:], empty], axis=0)
        beside = beside + jnp.where(lane == 0, 0.0, pltpu.roll(v, 1, 1))
        beside = beside + jnp.where(lane == LANES - 1, 0.0, pltpu.roll(v, LANES - 1, 1))
        return v, (6.0 + diag[x]) * v - beside

    me = (gx * 8 + gy) * 4 + gz
    lower_half = lax.broadcasted_iota(jnp.int32, (1, LANES), 1) < LANES // 2

    def start_sum(it, rz, wz):
        rows = [jnp.sum(v, axis=0, keepdims=True) for v in (rz, wz)]
        rows = [row + pltpu.roll(row, LANES // 2, 1) for row in rows]
        sums[it, pl.ds(me, 1), :] = jnp.where(lower_half, rows[0], rows[1])
        for peer in everyone:
            pltpu.make_async_remote_copy(
                sums.at[it, me], sums.at[it, me], sum_send.at[it], sum_recv.at[it],
                device_id=peer, device_id_type=MESH,
            ).start()

    def totals(it):
        some = sums.at[it, pl.ds(0, DEVICES - 1)]
        pltpu.make_async_copy(some, some, sum_recv.at[it]).wait()
        total = jnp.sum(sums[it], axis=0, keepdims=True)
        rz = jnp.sum(jnp.where(lower_half, total, 0.0), keepdims=True)
        wz = jnp.sum(jnp.where(lower_half, 0.0, total), keepdims=True)
        return [jnp.broadcast_to(v, (8, LANES)) for v in (rz, wz)]

    def folded(v):
        return jnp.sum(tiled(v), axis=0)

    def many(body):
        def some(i, carry):
            for j in range(UNROLL):
                carry = body(i * UNROLL + j, carry)
            return carry

        return some

    def rows_of(c, body, carry):
        begin = c * (CHUNK // UNROLL)
        return lax.fori_loop(begin, begin + CHUNK // UNROLL, many(body), carry)

    zero = jnp.zeros((8, LANES), f32)

    def ordered(i):
        return 3 * i - (i // 2) * (2 * i + 1)

    def blocks_pass(it, source, target, before):
        def body(i, carry):
            c = ordered(i)
            before(i, c)
            apply_blocks(source, target, it, c)

            @pl.when(i == 1)
            def _():
                start_halo(target, it, along_rows)

            return carry

        lax.fori_loop(0, STEPS, body, 0)
        start_halo(target, it, along_lanes)

    def arrived(array, target):
        def wait(i, c):
            some = target.at[pl.ds(pl.multiple_of(c * CHUNK, CHUNK), CHUNK)]
            pltpu.make_async_copy(some, some, col_sem.at[array, c]).wait()

        return wait

    def first_ready(i, c):
        spread(i)
        arrived(0, res)(i, c)

    blocks_pass(0, res, u0, first_ready)
    spread(STEPS)
    for c in ORDER[2:]:
        send_columns(1, diagonal, diag, c)
    wait_halo(u0, 0, along_rows)
    wait_halo(u0, 0, along_lanes)
    set_border(0)

    def first_image(i, carry):
        c = ordered(i)
        arrived(1, diag)(i, c)

        def body(x, carry):
            rz, wz = carry
            u, w = stencil(u0, x)
            w = w - beyond(x)
            w0[x] = w
            return rz + folded(res[x] * u), wz + folded(w * u)

        return rows_of(c, body, carry)

    start_sum(0, *lax.fori_loop(0, STEPS, first_image, (zero, zero)))

    def image_pass(it, array, target):
        def body(x, carry):
            _, target[x] = stencil(array, x)
            return carry

        lax.fori_loop(CHUNK // UNROLL, (ROWS - CHUNK) // UNROLL, many(body), 0)
        wait_halo(array, it, along_rows)
        rows_of(0, body, 0)
        rows_of(STEPS - 1, body, 0)

    blocks_pass(1, w0, m0, lambda i, c: None)
    image_pass(1, m0, n0)
    wait_halo(m0, 1, along_lanes)
    set_border(1)
    rz0, wz0 = totals(0)
    alpha0 = rz0 / wz0

    def second(x, carry):
        rz, wz = carry
        n = n0[x] - beyond(x)
        n0[x] = n
        w = tiled(w0[x])
        r = tiled(res[x]) - alpha0 * w
        u = tiled(u0[x + 1]) - alpha0 * tiled(m0[x + 1])
        w = w - alpha0 * tiled(n)
        w1[x] = flat(w)
        return rz + jnp.sum(r * u, axis=0), wz + jnp.sum(w * u, axis=0)

    start_sum(1, *lax.fori_loop(0, ROWS // UNROLL, many(second), (zero, zero)))
    blocks_pass(2, w1, m1, lambda i, c: None)
    image_pass(2, m1, n1)
    wait_halo(m1, 2, along_lanes)
    set_border(2)
    rz1, wz1 = totals(1)
    beta1 = rz1 / rz0
    alpha1 = rz1 / (wz1 - beta1 * rz1 / alpha0)

    def third(x, carry):
        rz, wz = carry
        n = n1[x] - beyond(x)
        first_w, second_w = tiled(w0[x]), tiled(w1[x])
        r = tiled(res[x]) - alpha0 * first_w - alpha1 * (second_w + beta1 * first_w)
        second_m = tiled(m0[x + 1])
        u = tiled(u0[x + 1]) - alpha0 * second_m - alpha1 * (tiled(m1[x + 1]) + beta1 * second_m)
        w = second_w - alpha1 * (tiled(n) + beta1 * tiled(n0[x]))
        return rz + jnp.sum(r * u, axis=0), wz + jnp.sum(w * u, axis=0)

    start_sum(2, *lax.fori_loop(0, ROWS // UNROLL, many(third), (zero, zero)))
    rz2, wz2 = totals(2)
    beta2 = rz2 / rz1
    alpha2 = rz2 / (wz2 - beta2 * rz2 / alpha1)

    by_u = alpha0 + alpha1 * (1.0 + beta1) + alpha2 * (1.0 + beta2 * (1.0 + beta1))
    by_m = -alpha1 * alpha0 - alpha2 * (alpha0 + alpha1 * beta1 + beta2 * alpha0)
    by_n = -alpha2 * alpha1

    def joined(u, m, n):
        return flat(by_u * tiled(u) + by_m * tiled(m) + by_n * tiled(n))

    def last_rows(x, carry):
        fin[x] = joined(u0[x], m0[x], m1[x])
        return carry

    lax.fori_loop(0, (ROWS + 2) // 6, lambda i, k: [last_rows(6 * i + j, k) for j in range(6)][0], 0)
    sides[...] = joined(*[jnp.where(even, left[it], right[it]) for it in range(3)])

    mine = pl.ds(pl.multiple_of(part * ROWS, ROWS), ROWS)
    inner = fin.at[pl.ds(1, ROWS)]

    def give(k, source, target, recv):
        pltpu.make_async_remote_copy(
            source, target, out_send, recv, device_id={"gz": k}, device_id_type=MESH
        ).start()

    def keep(source, target, recv):
        pltpu.make_async_copy(source, target, recv).start()

    for j in range(1, 4):
        k = lax.rem(gz + j, 4)
        near = pl.ds(pl.multiple_of(k * SLAB, SLAB), SLAB)
        give(k, sides.at[near], out_sides.at[part], sides_recv)
        for end, here in enumerate((part == 0, part == 3)):
            row = end * (ROWS + 1)
            pl.when(here)(functools.partial(give, k, fin.at[row, near], out_ends.at[end], ends_recv))

        @pl.when(k > 0)
        def _():
            give(k, inner.at[:, k * SLAB - 1, :], out_sol.at[0, mine, :], out_recv)

        @pl.when(k < 3)
        def _():
            give(k, inner.at[:, k * SLAB + SLAB, :], out_sol.at[SLAB + 1, mine, :], out_recv)

    def send_back(d, carry):
        for j in range(1, 4):
            k = lax.rem(gz + j, 4)
            give(k, inner.at[:, k * SLAB + d, :], out_sol.at[d + 1, mine, :], out_recv)
        return carry

    lax.fori_loop(0, SLAB, send_back, 0)

    near = pl.ds(base, SLAB)
    keep(sides.at[near], out_sides.at[part], sides_recv)
    for end, here in enumerate((part == 0, part == 3)):
        row = end * (ROWS + 1)
        pl.when(here)(functools.partial(keep, fin.at[row, near], out_ends.at[end], ends_recv))

    def keep_own(d, carry):
        keep(inner.at[:, base + d, :], out_sol.at[d + 1, mine, :], out_recv)
        return carry

    lax.fori_loop(0, SLAB, keep_own, 0)
    for outside, plane, depth in ((gz == 0, 0, base - 1), (gz == 3, SLAB + 1, base + SLAB)):

        @pl.when(jnp.logical_not(outside))
        def _():
            keep(inner.at[:, depth, :], out_sol.at[plane, mine, :], out_recv)

        @pl.when(outside)
        def _():
            for k in range(4):
                keep(blank, out_sol.at[plane, pl.ds(k * ROWS, ROWS), :], out_recv)

    some = res.at[pl.ds(0, 3 * SLAB)]
    for array in range(2):
        pltpu.make_async_copy(some, some, in_send.at[array]).wait()
    for it, array in enumerate((u0, m0, m1)):
        for sends, _, copy in halo_copies(array, it):
            pl.when(sends)(lambda: copy().wait_send())
        group = sums.at[it, pl.ds(0, DEVICES - 1)]
        pltpu.make_async_copy(group, group, sum_send.at[it]).wait()
    for target, recv in ((out_sides, sides_recv), (out_ends, ends_recv), (out_sol, out_recv)):
        pltpu.make_async_copy(target, target, recv).wait()
    pltpu.make_async_copy(some, some, out_send).wait()
    pltpu.make_async_copy(sides.at[pl.ds(0, 3 * SLAB)], sides.at[pl.ds(0, 3 * SLAB)], out_send).wait()
    for _ in range(4):
        pltpu.make_async_copy(blank, blank, out_send).wait()

    @pl.when(jnp.logical_or(gz == 0, gz == 3))
    def _():
        pltpu.make_async_copy(blank, blank, out_send).wait()

    @pl.when(jnp.logical_or(part == 0, part == 3))
    def _():
        some_rows = blank.at[pl.ds(0, 3 * SLAB)]
        pltpu.make_async_copy(some_rows, some_rows, out_send).wait()


def residual_kernel(
    right_side, diagonal, inner, sides, ends, out_sol, out_res,
    sol, rhs, diag, res, side, end, whole, turned, load, store,
):
    groups = SLAB // GROUP
    own = [pl.ds(g * GROUP, GROUP) for g in range(groups)]
    copies = [
        pltpu.make_async_copy(sides, side, load.at[2 * groups]),
        pltpu.make_async_copy(ends, end, load.at[2 * groups + 1]),
    ]
    planes, others = [], []
    for g in range(groups):
        begin = g * GROUP + (2 if g else 0)
        some = pl.ds(begin, GROUP + (0 if g else 2))
        planes.append(pltpu.make_async_copy(inner.at[some], sol.at[some], load.at[g]))
        others.append(
            [
                pltpu.make_async_copy(right_side.at[own[g]], rhs.at[own[g]], load.at[groups + g]),
                pltpu.make_async_copy(diagonal.at[own[g]], diag.at[own[g]], load.at[2 * groups + 2 + g]),
            ]
        )
    for copy in copies + [planes[0]] + others[0]:
        copy.start()
    for g in range(1, groups):
        for copy in [planes[g]] + others[g]:
            copy.start()
    for copy in copies:
        copy.wait()
    whole[...] = jnp.concatenate([side[...].reshape(DEEP, LANES), jnp.zeros((DEEP, LANES), f32)], axis=0).T
    for k in range(2):
        turned[k] = whole[pl.ds(k, ROWS, stride=2), :]
    lane = lax.broadcasted_iota(jnp.int32, (ROWS, LANES), 1)

    def plane(d, carry):
        for t in range(4):
            begin = t * ROWS
            rows = pl.ds(begin, ROWS)
            v = sol[d + 1, rows, :]
            beside = sol[d, rows, :] + sol[d + 2, rows, :]
            before = end[0, pl.ds(d, 1), :] if t == 0 else sol[d + 1, pl.ds(begin - 1, 1), :]
            after = end[1, pl.ds(d, 1), :] if t == 3 else sol[d + 1, pl.ds(begin + ROWS, 1), :]
            beside = beside + jnp.concatenate([before, v[:-1]], axis=0)
            beside = beside + jnp.concatenate([v[1:], after], axis=0)
            spot = t * SLAB + d
            from_left = pltpu.roll(turned[0], lax.rem(LANES - spot, LANES), 1)
            from_right = pltpu.roll(turned[1], LANES - 1 - spot, 1)
            beside = beside + jnp.where(lane == 0, from_left, pltpu.roll(v, 1, 1))
            beside = beside + jnp.where(lane == LANES - 1, from_right, pltpu.roll(v, LANES - 1, 1))
            res[d, rows, :] = rhs[d, rows, :] - ((6.0 + diag[d, rows, :]) * v - beside)
        return carry

    stores = []
    for g in range(groups):
        for copy in [planes[g]] + others[g]:
            copy.wait()
        lax.fori_loop(g * GROUP, (g + 1) * GROUP, plane, 0)
        stores += [
            pltpu.make_async_copy(res.at[own[g]], out_res.at[own[g]], store.at[0, g]),
            pltpu.make_async_copy(
                sol.at[pl.ds(g * GROUP + 1, GROUP)], out_sol.at[own[g]], store.at[1, g]
            ),
        ]
        for copy in stores[-2:]:
            copy.start()
    for copy in stores:
        copy.wait()


def per_device(right_side, diagonal, regime, inverses):
    shape = jax.ShapeDtypeStruct(right_side.shape, f32)
    field = pltpu.VMEM((ROWS, DEEP, LANES), f32)
    padded = pltpu.VMEM((ROWS + 2, DEEP, LANES), f32)
    plane = (DEEP, LANES)
    anywhere = pl.BlockSpec(memory_space=pl.ANY)
    wide = (SLAB + 2,) + right_side.shape[1:]
    inner, sides, ends = pl.pallas_call(
        kernel,
        out_shape=(
            jax.ShapeDtypeStruct(wide, f32),
            jax.ShapeDtypeStruct((4, SLAB, LANES), f32),
            jax.ShapeDtypeStruct((2, SLAB, LANES), f32),
        ),
        in_specs=[anywhere] * 4,
        out_specs=[anywhere] * 3,
        scratch_shapes=[
            field, field, padded, padded, padded, field, field, field, field, padded,
            pltpu.VMEM((ROWS, LANES), jnp.int32),
            pltpu.VMEM((NREG * DEEP, DEEP), f32),
            pltpu.VMEM((NREG * DEEP, 4 * DEEP), bf16),
            pltpu.VMEM((3,) + plane, f32),
            pltpu.VMEM((3,) + plane, f32),
            pltpu.VMEM((3,) + plane, f32),
            pltpu.VMEM(plane, f32),
            pltpu.VMEM(plane, f32),
            pltpu.VMEM(plane, f32),
            pltpu.VMEM((3, DEVICES, LANES), f32),
            pltpu.SemaphoreType.REGULAR((STEPS + 1,)),
            pltpu.SemaphoreType.DMA((2, STEPS)),
            pltpu.SemaphoreType.DMA((2,)),
            pltpu.SemaphoreType.DMA((2,)),
            pltpu.SemaphoreType.DMA((3, 4)),
            pltpu.SemaphoreType.DMA((3, 4)),
            pltpu.SemaphoreType.DMA((3,)),
            pltpu.SemaphoreType.DMA((3,)),
            pltpu.SemaphoreType.DMA,
            pltpu.SemaphoreType.DMA,
            pltpu.SemaphoreType.DMA,
            pltpu.SemaphoreType.DMA,
        ],
        compiler_params=pltpu.CompilerParams(
            collective_id=0, has_side_effects=True, vmem_limit_bytes=60 * 2**20
        ),
    )(right_side, diagonal, regime, inverses.reshape(NREG * DEEP, DEEP))
    slab = pltpu.VMEM(right_side.shape, f32)
    groups = SLAB // GROUP
    return pl.pallas_call(
        residual_kernel,
        out_shape=(shape, shape),
        in_specs=[anywhere] * 5,
        out_specs=[anywhere] * 2,
        scratch_shapes=[
            pltpu.VMEM(wide, f32), slab, slab, slab,
            pltpu.VMEM((4, SLAB, LANES), f32),
            pltpu.VMEM((2, SLAB, LANES), f32),
            pltpu.VMEM((LANES, LANES), f32),
            pltpu.VMEM((2, ROWS, LANES), f32),
            pltpu.SemaphoreType.DMA((3 * groups + 2,)),
            pltpu.SemaphoreType.DMA((2, groups)),
        ],
        compiler_params=pltpu.CompilerParams(vmem_limit_bytes=60 * 2**20),
    )(right_side, diagonal, inner, sides, ends)


def solution(mesh):
    field = P("gz", "gx", "gy")
    return jax.shard_map(
        per_device,
        mesh=mesh,
        in_specs=(field, field, P("gx", "gy"), P()),
        out_specs=(field, field),
        check_vma=False,
    )
```

```python
import functools

import jax
import jax.numpy as jnp
from jax import lax
from jax.experimental import pallas as pl
from jax.experimental.pallas import tpu as pltpu
from jax.sharding import PartitionSpec as P

f32 = jnp.float32
bf16 = jnp.bfloat16
MESH = pl.DeviceIdType.MESH
NREG = 8
ROWS = 64
DEEP = 64
SLAB = 16
LANES = 128
CHUNK = 16
STEPS = ROWS // CHUNK
DEVICES = 128
ORDER = (0, 3, 1, 2)
EARLY = 16
UNROLL = 16
GROUP = 4


def halves(v):
    high = v.astype(bf16)
    return high, (v - high.astype(f32)).astype(bf16)


def tiled(v):
    return v.reshape(DEEP // 8, 8, LANES)


def flat(v):
    return v.reshape(DEEP, LANES)


def kernel(
    right_side, diagonal, regime, blocks,
    out_sol, out_early, out_sides, out_ends, weights,
    res, diag, u0, m0, m1, w0, n0, n1, w1, fin,
    reg, inv, stack, edge, left, right, border, sides, blank, sums,
    rounds, col_sem, in_send, small_sem, halo_recv, halo_send, sum_recv, sum_send, early_recv, early_send, out_recv, sides_recv, ends_recv, out_send,
):
    gx, gy, gz = lax.axis_index("gx"), lax.axis_index("gy"), lax.axis_index("gz")
    odd = lax.rem(gx, 2)
    part = gz + odd * (3 - 2 * gz)
    stride = 1 - 2 * odd
    first, last = (3 - part) // 3, part // 3
    line = gx * 4 + part
    lower = {"gx": gx - first, "gz": gz - stride * (1 - first)}
    upper = {"gx": gx + last, "gz": gz + stride * (1 - last)}
    has_lower, has_upper = line > 0, line < 15
    has_left, has_right = gy > 0, gy < 7

    everyone = [
        {"gx": lax.rem(gx + a, 4), "gy": lax.rem(gy + b, 8), "gz": lax.rem(gz + c, 4)}
        for a in (2, 1, 3, 0) for b in (4, 3, 5, 2, 6, 1, 7, 0) for c in (2, 3, 1, 0)
    ][:-1]
    barrier = pltpu.get_barrier_semaphore()
    layer, side, slot, core = gy // 2, lax.rem(gy, 2), gz // 2, lax.rem(gz, 2)
    near_by = [{"gz": lax.rem(gz + j, 4)} for j in (1, 2, 3)]
    near_by += [{"gx": lax.rem(gx + j, 4)} for j in (1, 3)]
    near_by += [{"gy": lax.rem(gy + j, 8)} for j in (2, 6)]
    near_by += [{"gy": 2 * layer + 1 - side, "gz": 2 * (1 - slot) + core}]

    def tell(semaphore):
        for peer in near_by:
            pl.semaphore_signal(semaphore, inc=1, device_id=peer, device_id_type=MESH)

    def spread(k):
        tell(rounds.at[k])
        pl.semaphore_wait(rounds.at[k], len(near_by))

    tell(barrier)

    small = [
        pltpu.make_async_copy(blocks, inv, small_sem.at[0]),
        pltpu.make_async_copy(
            regime.at[pl.ds(pl.multiple_of(part * ROWS, ROWS), ROWS), :], reg, small_sem.at[1]
        ),
    ]
    for copy in small:
        copy.start()
    base = pl.multiple_of(gz * SLAB, SLAB)

    def part_of(k):
        return k + odd * (3 - 2 * k)

    def send_columns(array, source, target, c):
        def body(d, carry):
            rows = pl.ds(c * CHUNK, CHUNK)
            for j in range(1, 4):
                k = lax.rem(gz + j, 4)
                begin = pl.multiple_of(part_of(k) * ROWS + c * CHUNK, CHUNK)
                pltpu.make_async_remote_copy(
                    source.at[d, pl.ds(begin, CHUNK), :],
                    target.at[rows, base + d, :],
                    in_send.at[array],
                    col_sem.at[array, c],
                    device_id={"gz": k},
                    device_id_type=MESH,
                ).start()
            begin = pl.multiple_of(part * ROWS + c * CHUNK, CHUNK)
            pltpu.make_async_copy(
                source.at[d, pl.ds(begin, CHUNK), :],
                target.at[rows, base + d, :],
                col_sem.at[array, c],
            ).start()
            return carry

        lax.fori_loop(0, SLAB, body, 0)

    pl.semaphore_wait(barrier, len(near_by))
    for c in ORDER:
        send_columns(0, right_side, res, c)
    for c in ORDER[:2]:
        send_columns(1, diagonal, diag, c)

    nothing = jnp.zeros((DEEP, LANES), f32)
    blank[...] = nothing
    for array in (u0, m0, m1):

        @pl.when(line == 0)
        def _():
            array[0] = nothing

        @pl.when(line == 15)
        def _():
            array[ROWS + 1] = nothing

    for it in range(3):

        @pl.when(gy == 0)
        def _():
            left[it] = nothing

        @pl.when(gy == 7)
        def _():
            right[it] = nothing

        edge[it] = nothing

    for copy in small:
        copy.wait()
    high, low = halves(inv[...])
    stack[...] = jnp.concatenate([high, high, low, low], axis=1)

    lane = lax.broadcasted_iota(jnp.int32, (DEEP, LANES), 1)

    def apply_blocks(source, target, it, c):
        ends = edge[it]
        for h in range(CHUNK // 2):
            x = c * CHUNK + 2 * h
            both = jnp.concatenate([source[x], source[x + 1]], axis=1)
            high, low = halves(both)
            out = jnp.dot(
                stack[...],
                jnp.concatenate([high, low, high, low], axis=0),
                preferred_element_type=f32,
            )
            kind = jnp.concatenate([reg[pl.ds(x, 1), :], reg[pl.ds(x + 1, 1), :]], axis=1)
            kind = jnp.broadcast_to(kind, (DEEP, 2 * LANES))
            some = [out[k * DEEP : (k + 1) * DEEP] for k in range(NREG)]
            for bit in range(3):
                chosen = (kind & (1 << bit)) != 0
                some = [jnp.where(chosen, some[i + 1], some[i]) for i in range(0, len(some), 2)]
            for j in range(2):
                z = some[0][:, j * LANES : (j + 1) * LANES]
                target[x + j + 1] = z
                turned = pltpu.roll(z, 2 * (x + j) + 1, 1)
                ends = jnp.where((lane == 2 * (x + j)) | (lane == 2 * (x + j) + 1), turned, ends)
        edge[it] = ends

    def halo_copies(array, it):
        def copy(k, source, target, device):
            return pltpu.make_async_remote_copy(
                source, target, halo_send.at[it, k], halo_recv.at[it, k],
                device_id=device, device_id_type=MESH,
            )

        copy = functools.partial(functools.partial, copy)
        return (
            (has_lower, has_upper, copy(0, array.at[1], array.at[ROWS + 1], lower)),
            (has_upper, has_lower, copy(1, array.at[ROWS], array.at[0], upper)),
            (has_left, has_right, copy(2, edge.at[it], right.at[it], {"gy": gy - 1})),
            (has_right, has_left, copy(3, edge.at[it], left.at[it], {"gy": gy + 1})),
        )

    def start_halo(array, it, which):
        for sends, _, copy in halo_copies(array, it)[which]:
            pl.when(sends)(lambda: copy().start())

    def wait_halo(array, it, which):
        for _, receives, copy in halo_copies(array, it)[which]:
            pl.when(receives)(lambda: copy().wait_recv())

    along_rows, along_lanes = slice(0, 2), slice(2, 4)
    even = lax.rem(lane, 2) == 0
    outer = (lane == 0) | (lane == LANES - 1)

    def set_border(it):
        border[...] = jnp.where(even, left[it], pltpu.roll(right[it], LANES - 2, 1))

    def beyond(x):
        turned = pltpu.roll(border[...], lax.rem(LANES - 2 * x, LANES), 1)
        return jnp.where(outer, turned, 0.0)

    def stencil(array, x):
        v = array[x + 1]
        beside = array[x] + array[x + 2]
        empty = jnp.zeros((1, LANES), f32)
        beside = beside + jnp.concatenate([empty, v[:-1]], axis=0)
        beside = beside + jnp.concatenate([v[1:], empty], axis=0)
        beside = beside + jnp.where(lane == 0, 0.0, pltpu.roll(v, 1, 1))
        beside = beside + jnp.where(lane == LANES - 1, 0.0, pltpu.roll(v, LANES - 1, 1))
        return v, (6.0 + diag[x]) * v - beside

    me = (gx * 8 + gy) * 4 + gz
    lower_half = lax.broadcasted_iota(jnp.int32, (1, LANES), 1) < LANES // 2

    def start_sum(it, rz, wz):
        rows = [jnp.sum(v, axis=0, keepdims=True) for v in (rz, wz)]
        rows = [row + pltpu.roll(row, LANES // 2, 1) for row in rows]
        sums[it, pl.ds(me, 1), :] = jnp.where(lower_half, rows[0], rows[1])
        for peer in everyone:
            pltpu.make_async_remote_copy(
                sums.at[it, me], sums.at[it, me], sum_send.at[it], sum_recv.at[it],
                device_id=peer, device_id_type=MESH,
            ).start()

    def totals(it):
        some = sums.at[it, pl.ds(0, DEVICES - 1)]
        pltpu.make_async_copy(some, some, sum_recv.at[it]).wait()
        total = jnp.sum(sums[it], axis=0, keepdims=True)
        rz = jnp.sum(jnp.where(lower_half, total, 0.0), keepdims=True)
        wz = jnp.sum(jnp.where(lower_half, 0.0, total), keepdims=True)
        return [jnp.broadcast_to(v, (8, LANES)) for v in (rz, wz)]

    def folded(v):
        return jnp.sum(tiled(v), axis=0)

    def many(body):
        def some(i, carry):
            for j in range(UNROLL):
                carry = body(i * UNROLL + j, carry)
            return carry

        return some

    def rows_of(c, body, carry):
        begin = c * (CHUNK // UNROLL)
        return lax.fori_loop(begin, begin + CHUNK // UNROLL, many(body), carry)

    zero = jnp.zeros((8, LANES), f32)

    def ordered(i):
        return 3 * i - (i // 2) * (2 * i + 1)

    def blocks_pass(it, source, target, before):
        def body(i, carry):
            c = ordered(i)
            before(i, c)
            apply_blocks(source, target, it, c)

            @pl.when(i == 1)
            def _():
                start_halo(target, it, along_rows)

            return carry

        lax.fori_loop(0, STEPS, body, 0)
        start_halo(target, it, along_lanes)

    def give(k, source, target, send, recv):
        pltpu.make_async_remote_copy(
            source, target, send, recv, device_id={"gz": k}, device_id_type=MESH
        ).start()

    def keep(source, target, recv):
        pltpu.make_async_copy(source, target, recv).start()

    def deliver(source, target, pitch, offset, count, send, recv):
        here = pl.ds(pl.multiple_of(part * pitch + offset, 8), count)

        def plane(d, carry):
            for j in range(1, 4):
                k = lax.rem(gz + j, 4)
                give(k, source.at[:, k * SLAB + d, :], target.at[d + 1, here, :], send, recv)
            keep(source.at[:, base + d, :], target.at[d + 1, here, :], recv)
            return carry

        for j in range(1, 4):
            k = lax.rem(gz + j, 4)

            @pl.when(k > 0)
            def _():
                give(k, source.at[:, k * SLAB - 1, :], target.at[0, here, :], send, recv)

            @pl.when(k < 3)
            def _():
                give(k, source.at[:, k * SLAB + SLAB, :], target.at[SLAB + 1, here, :], send, recv)

        lax.fori_loop(0, SLAB, plane, 0)
        for outside, plane_at, depth in ((gz == 0, 0, base - 1), (gz == 3, SLAB + 1, base + SLAB)):

            @pl.when(jnp.logical_not(outside))
            def _():
                keep(source.at[:, depth, :], target.at[plane_at, here, :], recv)

            @pl.when(outside)
            def _():
                for t in range(4):
                    keep(blank.at[pl.ds(0, count)], target.at[plane_at, pl.ds(t * pitch + offset, count), :], recv)

    def delivered(source, send):
        some, one = source.at[:, pl.ds(0, 3 * SLAB), :], source.at[:, 0, :]
        pltpu.make_async_copy(some, some, send).wait()
        for _ in range(4):
            pltpu.make_async_copy(one, one, send).wait()

        @pl.when((gz == 0) | (gz == 3))
        def _():
            pltpu.make_async_copy(one, one, send).wait()

    def early(it, array):
        some = array.at[pl.ds(1, EARLY)]
        deliver(some, out_early.at[it], EARLY, 0, EARLY, early_send.at[it], early_recv.at[it])

    def arrived(array, target):
        def wait(i, c):
            some = target.at[pl.ds(pl.multiple_of(c * CHUNK, CHUNK), CHUNK)]
            pltpu.make_async_copy(some, some, col_sem.at[array, c]).wait()

        return wait

    def first_ready(i, c):
        spread(i)
        arrived(0, res)(i, c)

    blocks_pass(0, res, u0, first_ready)
    spread(STEPS)
    for c in ORDER[2:]:
        send_columns(1, diagonal, diag, c)
    wait_halo(u0, 0, along_rows)
    wait_halo(u0, 0, along_lanes)
    set_border(0)

    def first_image(i, carry):
        c = ordered(i)
        arrived(1, diag)(i, c)

        def body(x, carry):
            rz, wz = carry
            u, w = stencil(u0, x)
            w = w - beyond(x)
            w0[x] = w
            return rz + folded(res[x] * u), wz + folded(w * u)

        return rows_of(c, body, carry)

    start_sum(0, *lax.fori_loop(0, STEPS, first_image, (zero, zero)))

    def image_pass(it, array, target):
        def body(x, carry):
            _, target[x] = stencil(array, x)
            return carry

        lax.fori_loop(CHUNK // UNROLL, (ROWS - CHUNK) // UNROLL, many(body), 0)
        wait_halo(array, it, along_rows)
        rows_of(0, body, 0)
        rows_of(STEPS - 1, body, 0)

    blocks_pass(1, w0, m0, lambda i, c: None)
    early(0, u0)
    image_pass(1, m0, n0)
    wait_halo(m0, 1, along_lanes)
    set_border(1)
    rz0, wz0 = totals(0)
    alpha0 = rz0 / wz0

    def second(x, carry):
        rz, wz = carry
        n = n0[x] - beyond(x)
        n0[x] = n
        w = tiled(w0[x])
        r = tiled(res[x]) - alpha0 * w
        u = tiled(u0[x + 1]) - alpha0 * tiled(m0[x + 1])
        w = w - alpha0 * tiled(n)
        w1[x] = flat(w)
        return rz + jnp.sum(r * u, axis=0), wz + jnp.sum(w * u, axis=0)

    start_sum(1, *lax.fori_loop(0, ROWS // UNROLL, many(second), (zero, zero)))
    blocks_pass(2, w1, m1, lambda i, c: None)
    early(1, m0)
    image_pass(2, m1, n1)
    wait_halo(m1, 2, along_lanes)
    set_border(2)
    rz1, wz1 = totals(1)
    beta1 = rz1 / rz0
    alpha1 = rz1 / (wz1 - beta1 * rz1 / alpha0)

    def third(x, carry):
        rz, wz = carry
        n = n1[x] - beyond(x)
        first_w, second_w = tiled(w0[x]), tiled(w1[x])
        r = tiled(res[x]) - alpha0 * first_w - alpha1 * (second_w + beta1 * first_w)
        second_m = tiled(m0[x + 1])
        u = tiled(u0[x + 1]) - alpha0 * second_m - alpha1 * (tiled(m1[x + 1]) + beta1 * second_m)
        w = second_w - alpha1 * (tiled(n) + beta1 * tiled(n0[x]))
        return rz + jnp.sum(r * u, axis=0), wz + jnp.sum(w * u, axis=0)

    start_sum(2, *lax.fori_loop(0, ROWS // UNROLL, many(third), (zero, zero)))
    early(2, m1)
    rz2, wz2 = totals(2)
    beta2 = rz2 / rz1
    alpha2 = rz2 / (wz2 - beta2 * rz2 / alpha1)

    by_u = alpha0 + alpha1 * (1.0 + beta1) + alpha2 * (1.0 + beta2 * (1.0 + beta1))
    by_m = -alpha1 * alpha0 - alpha2 * (alpha0 + alpha1 * beta1 + beta2 * alpha0)
    by_n = -alpha2 * alpha1
    for k, weight in enumerate((by_u, by_m, by_n)):
        weights[k] = weight

    def joined(u, m, n):
        return flat(by_u * tiled(u) + by_m * tiled(m) + by_n * tiled(n))

    def last_rows(x, carry):
        fin[x] = joined(u0[x], m0[x], m1[x])
        return carry

    lax.fori_loop(0, (ROWS + 2) // 6, lambda i, k: [last_rows(6 * i + j, k) for j in range(6)][0], 0)
    sides[...] = joined(*[jnp.where(even, left[it], right[it]) for it in range(3)])

    late = fin.at[pl.ds(EARLY + 1, ROWS - EARLY)]
    deliver(late, out_sol, ROWS, EARLY, ROWS - EARLY, out_send.at[0], out_recv)
    for j in range(1, 4):
        k = lax.rem(gz + j, 4)
        near = pl.ds(pl.multiple_of(k * SLAB, SLAB), SLAB)
        give(k, sides.at[near], out_sides.at[part], out_send.at[1], sides_recv)
        for end, here in enumerate((part == 0, part == 3)):
            row = end * (ROWS + 1)
            pl.when(here)(
                functools.partial(give, k, fin.at[row, near], out_ends.at[end], out_send.at[2], ends_recv)
            )
    near = pl.ds(base, SLAB)
    keep(sides.at[near], out_sides.at[part], sides_recv)
    for end, here in enumerate((part == 0, part == 3)):
        row = end * (ROWS + 1)
        pl.when(here)(functools.partial(keep, fin.at[row, near], out_ends.at[end], ends_recv))

    some = res.at[pl.ds(0, 3 * SLAB)]
    for array in range(2):
        pltpu.make_async_copy(some, some, in_send.at[array]).wait()
    for it, array in enumerate((u0, m0, m1)):
        for sends, _, copy in halo_copies(array, it):
            pl.when(sends)(lambda: copy().wait_send())
        group = sums.at[it, pl.ds(0, DEVICES - 1)]
        pltpu.make_async_copy(group, group, sum_send.at[it]).wait()
    for it, array in enumerate((u0, m0, m1)):
        delivered(array.at[pl.ds(1, EARLY)], early_send.at[it])
        pltpu.make_async_copy(out_early.at[it], out_early.at[it], early_recv.at[it]).wait()
    for target, recv in (
        (out_sides, sides_recv),
        (out_ends, ends_recv),
        (out_sol.at[:, pl.ds(0, 4 * (ROWS - EARLY)), :], out_recv),
    ):
        pltpu.make_async_copy(target, target, recv).wait()
    delivered(late, out_send.at[0])
    some = sides.at[pl.ds(0, 3 * SLAB)]
    pltpu.make_async_copy(some, some, out_send.at[1]).wait()

    @pl.when((part == 0) | (part == 3))
    def _():
        pltpu.make_async_copy(some, some, out_send.at[2]).wait()


def residual_kernel(
    right_side, diagonal, inner, terms, sides, ends, weights, out_sol, out_res,
    sol, term, rhs, diag, res, side, end, spots, turned, load, store,
):
    groups = SLAB // GROUP
    own = [pl.ds(g * GROUP, GROUP) for g in range(groups)]
    copies = [
        pltpu.make_async_copy(sides, side, load.at[0, groups]),
        pltpu.make_async_copy(ends, end, load.at[1, groups]),
    ]
    planes, others = [], []
    for g in range(groups):
        begin = g * GROUP + (2 if g else 0)
        some = pl.ds(begin, GROUP + (0 if g else 2))
        one = []
        for t in range(4):
            late = pl.ds(t * ROWS + EARLY, ROWS - EARLY)
            one.append(pltpu.make_async_copy(inner.at[some, late], sol.at[some, late], load.at[t, g]))
        for k in range(3):
            one.append(pltpu.make_async_copy(terms.at[k, some], term.at[k, some], load.at[4 + k, g]))
        planes.append(one)
        others.append(
            [
                pltpu.make_async_copy(right_side.at[own[g]], rhs.at[own[g]], load.at[7, g]),
                pltpu.make_async_copy(diagonal.at[own[g]], diag.at[own[g]], load.at[8, g]),
            ]
        )
    for copy in copies:
        copy.start()
    for g in range(groups):
        for copy in planes[g] + others[g]:
            copy.start()
    for copy in copies:
        copy.wait()
    lane = lax.broadcasted_iota(jnp.int32, (ROWS, LANES), 1)
    listed = side[...].reshape(DEEP, LANES)
    for k in range(2):
        spots[pl.ds(k, DEEP, stride=2), :] = listed
    spots[...] = spots[...].T
    halves_of = [spots[pl.ds(k, ROWS, stride=2), :] for k in range(2)]
    turned[...] = jnp.where(lax.rem(lane, 2) == 0, halves_of[0], pltpu.roll(halves_of[1], LANES - 2, 1))
    outer = (lane == 0) | (lane == LANES - 1)

    def join(d, carry):
        for t in range(4):
            rows = pl.ds(t * EARLY, EARLY)
            parts = [
                term[k, d, rows, :].reshape(EARLY // 8, 8, LANES) * weights[k] for k in range(3)
            ]
            total = parts[0] + parts[1] + parts[2]
            sol[d, pl.ds(t * ROWS, EARLY), :] = total.reshape(EARLY, LANES)
        return carry

    def plane(d, carry):
        for t in range(4):
            begin = t * ROWS
            rows = pl.ds(begin, ROWS)
            v = sol[d + 1, rows, :]
            beside = sol[d, rows, :] + sol[d + 2, rows, :]
            before = end[0, pl.ds(d, 1), :] if t == 0 else sol[d + 1, pl.ds(begin - 1, 1), :]
            after = end[1, pl.ds(d, 1), :] if t == 3 else sol[d + 1, pl.ds(begin + ROWS, 1), :]
            beside = beside + jnp.concatenate([before, v[:-1]], axis=0)
            beside = beside + jnp.concatenate([v[1:], after], axis=0)
            spot = t * SLAB + d
            beyond = pltpu.roll(turned[...], lax.rem(LANES - 2 * spot, LANES), 1)
            beside = beside + jnp.where(lane == 0, 0.0, pltpu.roll(v, 1, 1))
            beside = beside + jnp.where(lane == LANES - 1, 0.0, pltpu.roll(v, LANES - 1, 1))
            beside = beside + jnp.where(outer, beyond, 0.0)
            res[d, rows, :] = rhs[d, rows, :] - ((6.0 + diag[d, rows, :]) * v - beside)
        return carry

    stores = []
    for g in range(groups):
        for copy in planes[g] + others[g]:
            copy.wait()
        lax.fori_loop(g * GROUP + (2 if g else 0), (g + 1) * GROUP + 2, join, 0)
        lax.fori_loop(g * GROUP, (g + 1) * GROUP, plane, 0)
        stores += [
            pltpu.make_async_copy(res.at[own[g]], out_res.at[own[g]], store.at[0, g]),
            pltpu.make_async_copy(
                sol.at[pl.ds(g * GROUP + 1, GROUP)], out_sol.at[own[g]], store.at[1, g]
            ),
        ]
        for copy in stores[-2:]:
            copy.start()
    for copy in stores:
        copy.wait()


def per_device(right_side, diagonal, regime, inverses):
    shape = jax.ShapeDtypeStruct(right_side.shape, f32)
    field = pltpu.VMEM((ROWS, DEEP, LANES), f32)
    padded = pltpu.VMEM((ROWS + 2, DEEP, LANES), f32)
    plane = (DEEP, LANES)
    anywhere = pl.BlockSpec(memory_space=pl.ANY)
    wide = (SLAB + 2,) + right_side.shape[1:]
    few = (3, SLAB + 2, 4 * EARLY, LANES)
    inner, terms, sides, ends, weights = pl.pallas_call(
        kernel,
        out_shape=(
            jax.ShapeDtypeStruct(wide, f32),
            jax.ShapeDtypeStruct(few, f32),
            jax.ShapeDtypeStruct((4, SLAB, LANES), f32),
            jax.ShapeDtypeStruct((2, SLAB, LANES), f32),
            jax.ShapeDtypeStruct((3, 8, LANES), f32),
        ),
        in_specs=[anywhere] * 4,
        out_specs=[anywhere] * 4 + [pl.BlockSpec(memory_space=pltpu.VMEM)],
        scratch_shapes=[
            field, field, padded, padded, padded, field, field, field, field, padded,
            pltpu.VMEM((ROWS, LANES), jnp.int32),
            pltpu.VMEM((NREG * DEEP, DEEP), f32),
            pltpu.VMEM((NREG * DEEP, 4 * DEEP), bf16),
            pltpu.VMEM((3,) + plane, f32),
            pltpu.VMEM((3,) + plane, f32),
            pltpu.VMEM((3,) + plane, f32),
            pltpu.VMEM(plane, f32),
            pltpu.VMEM(plane, f32),
            pltpu.VMEM(plane, f32),
            pltpu.VMEM((3, DEVICES, LANES), f32),
            pltpu.SemaphoreType.REGULAR((STEPS + 1,)),
            pltpu.SemaphoreType.DMA((2, STEPS)),
            pltpu.SemaphoreType.DMA((2,)),
            pltpu.SemaphoreType.DMA((2,)),
            pltpu.SemaphoreType.DMA((3, 4)),
            pltpu.SemaphoreType.DMA((3, 4)),
            pltpu.SemaphoreType.DMA((3,)),
            pltpu.SemaphoreType.DMA((3,)),
            pltpu.SemaphoreType.DMA((3,)),
            pltpu.SemaphoreType.DMA((3,)),
            pltpu.SemaphoreType.DMA,
            pltpu.SemaphoreType.DMA,
            pltpu.SemaphoreType.DMA,
            pltpu.SemaphoreType.DMA((3,)),
        ],
        compiler_params=pltpu.CompilerParams(
            collective_id=0, has_side_effects=True, vmem_limit_bytes=60 * 2**20
        ),
    )(right_side, diagonal, regime, inverses.reshape(NREG * DEEP, DEEP))
    slab = pltpu.VMEM(right_side.shape, f32)
    groups = SLAB // GROUP
    return pl.pallas_call(
        residual_kernel,
        out_shape=(shape, shape),
        in_specs=[anywhere] * 6 + [pl.BlockSpec(memory_space=pltpu.VMEM)],
        out_specs=[anywhere] * 2,
        scratch_shapes=[
            pltpu.VMEM(wide, f32), pltpu.VMEM(few, f32), slab, slab, slab,
            pltpu.VMEM((4, SLAB, LANES), f32),
            pltpu.VMEM((2, SLAB, LANES), f32),
            pltpu.VMEM((LANES, LANES), f32),
            pltpu.VMEM((ROWS, LANES), f32),
            pltpu.SemaphoreType.DMA((9, groups + 1)),
            pltpu.SemaphoreType.DMA((2, groups)),
        ],
        compiler_params=pltpu.CompilerParams(vmem_limit_bytes=60 * 2**20),
    )(right_side, diagonal, inner, terms, sides, ends, weights)


def solution(mesh):
    field = P("gz", "gx", "gy")
    return jax.shard_map(
        per_device,
        mesh=mesh,
        in_specs=(field, field, P("gx", "gy"), P()),
        out_specs=(field, field),
        check_vma=False,
    )
```

```python
import functools

import jax
import jax.numpy as jnp
from jax import lax
from jax.experimental import pallas as pl
from jax.experimental.pallas import tpu as pltpu
from jax.sharding import PartitionSpec as P

f32 = jnp.float32
bf16 = jnp.bfloat16
MESH = pl.DeviceIdType.MESH
NREG = 8
ROWS = 64
DEEP = 64
SLAB = 16
LANES = 128
CHUNK = 16
STEPS = ROWS // CHUNK
DEVICES = 128
ORDER = (0, 3, 1, 2)
EARLY = 16
UNROLL = 16
GROUP = 4


def halves(v):
    high = v.astype(bf16)
    return high, (v - high.astype(f32)).astype(bf16)


def tiled(v):
    return v.reshape(DEEP // 8, 8, LANES)


def flat(v):
    return v.reshape(DEEP, LANES)


def kernel(
    right_side, diagonal, regime, blocks,
    out_sol, out_early, out_sides, out_ends, weights,
    res, diag, u0, m0, m1, w0, n0, n1, w1, fin,
    reg, inv, stack, edge, left, right, border, sides, blank, sums,
    rounds, col_sem, in_send, small_sem, halo_recv, halo_send, sum_recv, sum_send, early_recv, early_send, out_recv, sides_recv, ends_recv, out_send,
):
    gx, gy, gz = lax.axis_index("gx"), lax.axis_index("gy"), lax.axis_index("gz")
    odd = lax.rem(gx, 2)
    part = gz + odd * (3 - 2 * gz)
    stride = 1 - 2 * odd
    first, last = (3 - part) // 3, part // 3
    line = gx * 4 + part
    lower = {"gx": gx - first, "gz": gz - stride * (1 - first)}
    upper = {"gx": gx + last, "gz": gz + stride * (1 - last)}
    has_lower, has_upper = line > 0, line < 15
    has_left, has_right = gy > 0, gy < 7

    everyone = [
        {"gx": lax.rem(gx + a, 4), "gy": lax.rem(gy + b, 8), "gz": lax.rem(gz + c, 4)}
        for a in (2, 1, 3, 0) for b in (4, 3, 5, 2, 6, 1, 7, 0) for c in (2, 3, 1, 0)
    ][:-1]
    barrier = pltpu.get_barrier_semaphore()
    layer, side, slot, core = gy // 2, lax.rem(gy, 2), gz // 2, lax.rem(gz, 2)
    near_by = [{"gz": lax.rem(gz + j, 4)} for j in (1, 2, 3)]
    near_by += [{"gx": lax.rem(gx + j, 4)} for j in (1, 3)]
    near_by += [{"gy": lax.rem(gy + j, 8)} for j in (2, 6)]
    near_by += [{"gy": 2 * layer + 1 - side, "gz": 2 * (1 - slot) + core}]

    def tell(semaphore):
        for peer in near_by:
            pl.semaphore_signal(semaphore, inc=1, device_id=peer, device_id_type=MESH)

    def spread(k):
        tell(rounds.at[k])
        pl.semaphore_wait(rounds.at[k], len(near_by))

    tell(barrier)

    small = [
        pltpu.make_async_copy(blocks, inv, small_sem.at[0]),
        pltpu.make_async_copy(
            regime.at[pl.ds(pl.multiple_of(part * ROWS, ROWS), ROWS), :], reg, small_sem.at[1]
        ),
    ]
    for copy in small:
        copy.start()
    base = pl.multiple_of(gz * SLAB, SLAB)

    def part_of(k):
        return k + odd * (3 - 2 * k)

    def send_columns(array, source, target, c):
        def body(d, carry):
            rows = pl.ds(c * CHUNK, CHUNK)
            for j in range(1, 4):
                k = lax.rem(gz + j, 4)
                begin = pl.multiple_of(part_of(k) * ROWS + c * CHUNK, CHUNK)
                pltpu.make_async_remote_copy(
                    source.at[d, pl.ds(begin, CHUNK), :],
                    target.at[rows, base + d, :],
                    in_send.at[array],
                    col_sem.at[array, c],
                    device_id={"gz": k},
                    device_id_type=MESH,
                ).start()
            begin = pl.multiple_of(part * ROWS + c * CHUNK, CHUNK)
            pltpu.make_async_copy(
                source.at[d, pl.ds(begin, CHUNK), :],
                target.at[rows, base + d, :],
                col_sem.at[array, c],
            ).start()
            return carry

        lax.fori_loop(0, SLAB, body, 0)

    pl.semaphore_wait(barrier, len(near_by))
    for c in ORDER:
        send_columns(0, right_side, res, c)
    for c in ORDER[:2]:
        send_columns(1, diagonal, diag, c)

    nothing = jnp.zeros((DEEP, LANES), f32)
    blank[...] = nothing
    for array in (u0, m0, m1):

        @pl.when(line == 0)
        def _():
            array[0] = nothing

        @pl.when(line == 15)
        def _():
            array[ROWS + 1] = nothing

    for it in range(3):

        @pl.when(gy == 0)
        def _():
            left[it] = nothing

        @pl.when(gy == 7)
        def _():
            right[it] = nothing

        edge[it] = nothing

    for copy in small:
        copy.wait()
    high, low = halves(inv[...])
    stack[...] = jnp.concatenate([high, high, low, low], axis=1)

    lane = lax.broadcasted_iota(jnp.int32, (DEEP, LANES), 1)

    def apply_blocks(source, target, it, c):
        ends = edge[it]
        for h in range(CHUNK // 2):
            x = c * CHUNK + 2 * h
            both = jnp.concatenate([source[x], source[x + 1]], axis=1)
            high, low = halves(both)
            out = jnp.dot(
                stack[...],
                jnp.concatenate([high, low, high, low], axis=0),
                preferred_element_type=f32,
            )
            kind = jnp.concatenate([reg[pl.ds(x, 1), :], reg[pl.ds(x + 1, 1), :]], axis=1)
            kind = jnp.broadcast_to(kind, (DEEP, 2 * LANES))
            some = [out[k * DEEP : (k + 1) * DEEP] for k in range(NREG)]
            for bit in range(3):
                chosen = (kind & (1 << bit)) != 0
                some = [jnp.where(chosen, some[i + 1], some[i]) for i in range(0, len(some), 2)]
            for j in range(2):
                z = some[0][:, j * LANES : (j + 1) * LANES]
                target[x + j + 1] = z
                turned = pltpu.roll(z, 2 * (x + j) + 1, 1)
                ends = jnp.where((lane == 2 * (x + j)) | (lane == 2 * (x + j) + 1), turned, ends)
        edge[it] = ends

    def halo_copies(array, it):
        def copy(k, source, target, device):
            return pltpu.make_async_remote_copy(
                source, target, halo_send.at[it, k], halo_recv.at[it, k],
                device_id=device, device_id_type=MESH,
            )

        copy = functools.partial(functools.partial, copy)
        return (
            (has_lower, has_upper, copy(0, array.at[1], array.at[ROWS + 1], lower)),
            (has_upper, has_lower, copy(1, array.at[ROWS], array.at[0], upper)),
            (has_left, has_right, copy(2, edge.at[it], right.at[it], {"gy": gy - 1})),
            (has_right, has_left, copy(3, edge.at[it], left.at[it], {"gy": gy + 1})),
        )

    def start_halo(array, it, which):
        for sends, _, copy in halo_copies(array, it)[which]:
            pl.when(sends)(lambda: copy().start())

    def wait_halo(array, it, which):
        for _, receives, copy in halo_copies(array, it)[which]:
            pl.when(receives)(lambda: copy().wait_recv())

    along_rows, along_lanes = slice(0, 2), slice(2, 4)
    even = lax.rem(lane, 2) == 0
    outer = (lane == 0) | (lane == LANES - 1)

    def set_border(it):
        border[...] = jnp.where(even, left[it], pltpu.roll(right[it], LANES - 2, 1))

    def beyond(x):
        turned = pltpu.roll(border[...], lax.rem(LANES - 2 * x, LANES), 1)
        return jnp.where(outer, turned, 0.0)

    def stencil(array, x):
        v = array[x + 1]
        beside = array[x] + array[x + 2]
        empty = jnp.zeros((1, LANES), f32)
        beside = beside + jnp.concatenate([empty, v[:-1]], axis=0)
        beside = beside + jnp.concatenate([v[1:], empty], axis=0)
        beside = beside + jnp.where(lane == 0, 0.0, pltpu.roll(v, 1, 1))
        beside = beside + jnp.where(lane == LANES - 1, 0.0, pltpu.roll(v, LANES - 1, 1))
        return v, (6.0 + diag[x]) * v - beside

    me = (gx * 8 + gy) * 4 + gz
    lower_half = lax.broadcasted_iota(jnp.int32, (1, LANES), 1) < LANES // 2

    def start_sum(it, rz, wz):
        rows = [jnp.sum(v, axis=0, keepdims=True) for v in (rz, wz)]
        rows = [row + pltpu.roll(row, LANES // 2, 1) for row in rows]
        sums[it, pl.ds(me, 1), :] = jnp.where(lower_half, rows[0], rows[1])
        for peer in everyone:
            pltpu.make_async_remote_copy(
                sums.at[it, me], sums.at[it, me], sum_send.at[it], sum_recv.at[it],
                device_id=peer, device_id_type=MESH,
            ).start()

    def totals(it):
        some = sums.at[it, pl.ds(0, DEVICES - 1)]
        pltpu.make_async_copy(some, some, sum_recv.at[it]).wait()
        total = jnp.sum(sums[it], axis=0, keepdims=True)
        rz = jnp.sum(jnp.where(lower_half, total, 0.0), keepdims=True)
        wz = jnp.sum(jnp.where(lower_half, 0.0, total), keepdims=True)
        return [jnp.broadcast_to(v, (8, LANES)) for v in (rz, wz)]

    def folded(v):
        return jnp.sum(tiled(v), axis=0)

    def many(body, count=UNROLL):
        def some(i, carry):
            for j in range(count):
                carry = body(i * count + j, carry)
            return carry

        return some

    def rows_of(c, body, carry):
        begin = c * (CHUNK // UNROLL)
        return lax.fori_loop(begin, begin + CHUNK // UNROLL, many(body), carry)

    zero = jnp.zeros((8, LANES), f32)

    def ordered(i):
        return 3 * i - (i // 2) * (2 * i + 1)

    def blocks_pass(it, source, target, before):
        def body(i, carry):
            c = ordered(i)
            before(i, c)
            apply_blocks(source, target, it, c)

            @pl.when(i == 1)
            def _():
                start_halo(target, it, along_rows)

            return carry

        lax.fori_loop(0, STEPS, body, 0)
        start_halo(target, it, along_lanes)

    def give(k, source, target, send, recv):
        pltpu.make_async_remote_copy(
            source, target, send, recv, device_id={"gz": k}, device_id_type=MESH
        ).start()

    def keep(source, target, recv):
        pltpu.make_async_copy(source, target, recv).start()

    def deliver(source, target, pitch, offset, count, send, recv):
        here = pl.ds(pl.multiple_of(part * pitch + offset, 8), count)

        def plane(d, carry):
            for j in range(1, 4):
                k = lax.rem(gz + j, 4)
                give(k, source.at[:, k * SLAB + d, :], target.at[d + 1, here, :], send, recv)
            keep(source.at[:, base + d, :], target.at[d + 1, here, :], recv)
            return carry

        for j in range(1, 4):
            k = lax.rem(gz + j, 4)

            @pl.when(k > 0)
            def _():
                give(k, source.at[:, k * SLAB - 1, :], target.at[0, here, :], send, recv)

            @pl.when(k < 3)
            def _():
                give(k, source.at[:, k * SLAB + SLAB, :], target.at[SLAB + 1, here, :], send, recv)

        lax.fori_loop(0, SLAB, plane, 0)
        for outside, plane_at, depth in ((gz == 0, 0, base - 1), (gz == 3, SLAB + 1, base + SLAB)):

            @pl.when(jnp.logical_not(outside))
            def _():
                keep(source.at[:, depth, :], target.at[plane_at, here, :], recv)

            @pl.when(outside)
            def _():
                for t in range(4):
                    keep(blank.at[pl.ds(0, count)], target.at[plane_at, pl.ds(t * pitch + offset, count), :], recv)

    def delivered(source, send):
        some, one = source.at[:, pl.ds(0, 3 * SLAB), :], source.at[:, 0, :]
        pltpu.make_async_copy(some, some, send).wait()
        for _ in range(4):
            pltpu.make_async_copy(one, one, send).wait()

        @pl.when((gz == 0) | (gz == 3))
        def _():
            pltpu.make_async_copy(one, one, send).wait()

    def early(it, array):
        some = array.at[pl.ds(1, EARLY)]
        deliver(some, out_early.at[it], EARLY, 0, EARLY, early_send.at[it], early_recv.at[it])

    def arrived(array, target):
        def wait(i, c):
            some = target.at[pl.ds(pl.multiple_of(c * CHUNK, CHUNK), CHUNK)]
            pltpu.make_async_copy(some, some, col_sem.at[array, c]).wait()

        return wait

    def first_ready(i, c):
        spread(i)
        arrived(0, res)(i, c)

    blocks_pass(0, res, u0, first_ready)
    spread(STEPS)
    for c in ORDER[2:]:
        send_columns(1, diagonal, diag, c)
    wait_halo(u0, 0, along_rows)
    wait_halo(u0, 0, along_lanes)
    set_border(0)

    def first_image(i, carry):
        c = ordered(i)
        arrived(1, diag)(i, c)

        def body(x, carry):
            rz, wz = carry
            u, w = stencil(u0, x)
            w = w - beyond(x)
            w0[x] = w
            return rz + folded(res[x] * u), wz + folded(w * u)

        return rows_of(c, body, carry)

    start_sum(0, *lax.fori_loop(0, STEPS, first_image, (zero, zero)))

    def image_pass(it, array, target):
        def body(x, carry):
            _, target[x] = stencil(array, x)
            return carry

        for j in range(CHUNK, ROWS - CHUNK):
            body(j, 0)
        wait_halo(array, it, along_rows)
        rows_of(0, body, 0)
        rows_of(STEPS - 1, body, 0)

    blocks_pass(1, w0, m0, lambda i, c: None)
    early(0, u0)
    image_pass(1, m0, n0)
    wait_halo(m0, 1, along_lanes)
    set_border(1)
    rz0, wz0 = totals(0)
    alpha0 = rz0 / wz0

    def second(x, carry):
        rz, wz = carry
        n = n0[x] - beyond(x)
        n0[x] = n
        w = tiled(w0[x])
        r = tiled(res[x]) - alpha0 * w
        u = tiled(u0[x + 1]) - alpha0 * tiled(m0[x + 1])
        w = w - alpha0 * tiled(n)
        w1[x] = flat(w)
        return rz + jnp.sum(r * u, axis=0), wz + jnp.sum(w * u, axis=0)

    start_sum(1, *lax.fori_loop(0, ROWS // UNROLL, many(second), (zero, zero)))
    blocks_pass(2, w1, m1, lambda i, c: None)
    early(1, m0)
    image_pass(2, m1, n1)
    wait_halo(m1, 2, along_lanes)
    set_border(2)
    rz1, wz1 = totals(1)
    beta1 = rz1 / rz0
    alpha1 = rz1 / (wz1 - beta1 * rz1 / alpha0)

    def third(x, carry):
        rz, wz = carry
        n = n1[x] - beyond(x)
        first_w, second_w = tiled(w0[x]), tiled(w1[x])
        r = tiled(res[x]) - alpha0 * first_w - alpha1 * (second_w + beta1 * first_w)
        second_m = tiled(m0[x + 1])
        u = tiled(u0[x + 1]) - alpha0 * second_m - alpha1 * (tiled(m1[x + 1]) + beta1 * second_m)
        w = second_w - alpha1 * (tiled(n) + beta1 * tiled(n0[x]))
        return rz + jnp.sum(r * u, axis=0), wz + jnp.sum(w * u, axis=0)

    start_sum(2, *lax.fori_loop(0, ROWS // 8, many(third, 8), (zero, zero)))
    early(2, m1)
    rz2, wz2 = totals(2)
    beta2 = rz2 / rz1
    alpha2 = rz2 / (wz2 - beta2 * rz2 / alpha1)

    by_u = alpha0 + alpha1 * (1.0 + beta1) + alpha2 * (1.0 + beta2 * (1.0 + beta1))
    by_m = -alpha1 * alpha0 - alpha2 * (alpha0 + alpha1 * beta1 + beta2 * alpha0)
    by_n = -alpha2 * alpha1
    for k, weight in enumerate((by_u, by_m, by_n)):
        weights[k] = weight

    def joined(u, m, n):
        return flat(by_u * tiled(u) + by_m * tiled(m) + by_n * tiled(n))

    def last_rows(x, carry):
        fin[x] = joined(u0[x], m0[x], m1[x])
        return carry

    lax.fori_loop(0, (ROWS + 2) // 6, lambda i, k: [last_rows(6 * i + j, k) for j in range(6)][0], 0)
    sides[...] = joined(*[jnp.where(even, left[it], right[it]) for it in range(3)])

    late = fin.at[pl.ds(EARLY + 1, ROWS - EARLY)]
    for j in range(1, 4):
        k = lax.rem(gz + j, 4)
        near = pl.ds(pl.multiple_of(k * SLAB, SLAB), SLAB)
        give(k, sides.at[near], out_sides.at[part], out_send.at[1], sides_recv)
        for end, here in enumerate((part == 0, part == 3)):
            row = end * (ROWS + 1)
            pl.when(here)(
                functools.partial(give, k, fin.at[row, near], out_ends.at[end], out_send.at[2], ends_recv)
            )
    near = pl.ds(base, SLAB)
    keep(sides.at[near], out_sides.at[part], sides_recv)
    for end, here in enumerate((part == 0, part == 3)):
        row = end * (ROWS + 1)
        pl.when(here)(functools.partial(keep, fin.at[row, near], out_ends.at[end], ends_recv))

    deliver(late, out_sol, ROWS, EARLY, ROWS - EARLY, out_send.at[0], out_recv)

    some = res.at[pl.ds(0, 3 * SLAB)]
    for array in range(2):
        pltpu.make_async_copy(some, some, in_send.at[array]).wait()
    for it, array in enumerate((u0, m0, m1)):
        for sends, _, copy in halo_copies(array, it):
            pl.when(sends)(lambda: copy().wait_send())
        group = sums.at[it, pl.ds(0, DEVICES - 1)]
        pltpu.make_async_copy(group, group, sum_send.at[it]).wait()
    for it, array in enumerate((u0, m0, m1)):
        delivered(array.at[pl.ds(1, EARLY)], early_send.at[it])
        pltpu.make_async_copy(out_early.at[it], out_early.at[it], early_recv.at[it]).wait()
    for target, recv in (
        (out_sides, sides_recv),
        (out_ends, ends_recv),
        (out_sol.at[:, pl.ds(0, 4 * (ROWS - EARLY)), :], out_recv),
    ):
        pltpu.make_async_copy(target, target, recv).wait()
    delivered(late, out_send.at[0])
    some = sides.at[pl.ds(0, 3 * SLAB)]
    pltpu.make_async_copy(some, some, out_send.at[1]).wait()

    @pl.when((part == 0) | (part == 3))
    def _():
        pltpu.make_async_copy(some, some, out_send.at[2]).wait()


def residual_kernel(
    right_side, diagonal, inner, terms, sides, ends, weights, out_sol, out_res,
    sol, term, rhs, diag, res, side, end, spots, turned, load, store,
):
    groups = SLAB // GROUP
    own = [pl.ds(g * GROUP, GROUP) for g in range(groups)]
    copies = [
        pltpu.make_async_copy(sides, side, load.at[0, groups]),
        pltpu.make_async_copy(ends, end, load.at[1, groups]),
    ]
    planes, others = [], []
    for g in range(groups):
        begin = g * GROUP + (2 if g else 0)
        some = pl.ds(begin, GROUP + (0 if g else 2))
        one = []
        for t in range(4):
            late = pl.ds(t * ROWS + EARLY, ROWS - EARLY)
            one.append(pltpu.make_async_copy(inner.at[some, late], sol.at[some, late], load.at[t, g]))
        for k in range(3):
            one.append(pltpu.make_async_copy(terms.at[k, some], term.at[k, some], load.at[4 + k, g]))
        planes.append(one)
        others.append(
            [
                pltpu.make_async_copy(right_side.at[own[g]], rhs.at[own[g]], load.at[7, g]),
                pltpu.make_async_copy(diagonal.at[own[g]], diag.at[own[g]], load.at[8, g]),
            ]
        )
    for copy in copies:
        copy.start()
    for g in range(groups):
        for copy in planes[g] + others[g]:
            copy.start()
    for copy in copies:
        copy.wait()
    lane = lax.broadcasted_iota(jnp.int32, (ROWS, LANES), 1)
    listed = side[...].reshape(DEEP, LANES)
    for k in range(2):
        spots[pl.ds(k, DEEP, stride=2), :] = listed
    spots[...] = spots[...].T
    halves_of = [spots[pl.ds(k, ROWS, stride=2), :] for k in range(2)]
    turned[...] = jnp.where(lax.rem(lane, 2) == 0, halves_of[0], pltpu.roll(halves_of[1], LANES - 2, 1))
    outer = (lane == 0) | (lane == LANES - 1)

    def join(d, carry):
        for t in range(4):
            rows = pl.ds(t * EARLY, EARLY)
            parts = [
                term[k, d, rows, :].reshape(EARLY // 8, 8, LANES) * weights[k] for k in range(3)
            ]
            total = parts[0] + parts[1] + parts[2]
            sol[d, pl.ds(t * ROWS, EARLY), :] = total.reshape(EARLY, LANES)
        return carry

    def plane(d, carry):
        for t in range(4):
            begin = t * ROWS
            rows = pl.ds(begin, ROWS)
            v = sol[d + 1, rows, :]
            beside = sol[d, rows, :] + sol[d + 2, rows, :]
            before = end[0, pl.ds(d, 1), :] if t == 0 else sol[d + 1, pl.ds(begin - 1, 1), :]
            after = end[1, pl.ds(d, 1), :] if t == 3 else sol[d + 1, pl.ds(begin + ROWS, 1), :]
            beside = beside + jnp.concatenate([before, v[:-1]], axis=0)
            beside = beside + jnp.concatenate([v[1:], after], axis=0)
            spot = t * SLAB + d
            beyond = pltpu.roll(turned[...], lax.rem(LANES - 2 * spot, LANES), 1)
            beside = beside + jnp.where(lane == 0, 0.0, pltpu.roll(v, 1, 1))
            beside = beside + jnp.where(lane == LANES - 1, 0.0, pltpu.roll(v, LANES - 1, 1))
            beside = beside + jnp.where(outer, beyond, 0.0)
            res[d, rows, :] = rhs[d, rows, :] - ((6.0 + diag[d, rows, :]) * v - beside)
        return carry

    stores = []
    for g in range(groups):
        for copy in planes[g] + others[g]:
            copy.wait()
        lax.fori_loop(g * GROUP + (2 if g else 0), (g + 1) * GROUP + 2, join, 0)
        lax.fori_loop(g * GROUP, (g + 1) * GROUP, plane, 0)
        stores += [
            pltpu.make_async_copy(res.at[own[g]], out_res.at[own[g]], store.at[0, g]),
            pltpu.make_async_copy(
                sol.at[pl.ds(g * GROUP + 1, GROUP)], out_sol.at[own[g]], store.at[1, g]
            ),
        ]
        for copy in stores[-2:]:
            copy.start()
    for copy in stores:
        copy.wait()


def per_device(right_side, diagonal, regime, inverses):
    shape = jax.ShapeDtypeStruct(right_side.shape, f32)
    field = pltpu.VMEM((ROWS, DEEP, LANES), f32)
    padded = pltpu.VMEM((ROWS + 2, DEEP, LANES), f32)
    plane = (DEEP, LANES)
    anywhere = pl.BlockSpec(memory_space=pl.ANY)
    wide = (SLAB + 2,) + right_side.shape[1:]
    few = (3, SLAB + 2, 4 * EARLY, LANES)
    inner, terms, sides, ends, weights = pl.pallas_call(
        kernel,
        out_shape=(
            jax.ShapeDtypeStruct(wide, f32),
            jax.ShapeDtypeStruct(few, f32),
            jax.ShapeDtypeStruct((4, SLAB, LANES), f32),
            jax.ShapeDtypeStruct((2, SLAB, LANES), f32),
            jax.ShapeDtypeStruct((3, 8, LANES), f32),
        ),
        in_specs=[anywhere] * 4,
        out_specs=[anywhere] * 4 + [pl.BlockSpec(memory_space=pltpu.VMEM)],
        scratch_shapes=[
            field, field, padded, padded, padded, field, field, field, field, padded,
            pltpu.VMEM((ROWS, LANES), jnp.int32),
            pltpu.VMEM((NREG * DEEP, DEEP), f32),
            pltpu.VMEM((NREG * DEEP, 4 * DEEP), bf16),
            pltpu.VMEM((3,) + plane, f32),
            pltpu.VMEM((3,) + plane, f32),
            pltpu.VMEM((3,) + plane, f32),
            pltpu.VMEM(plane, f32),
            pltpu.VMEM(plane, f32),
            pltpu.VMEM(plane, f32),
            pltpu.VMEM((3, DEVICES, LANES), f32),
            pltpu.SemaphoreType.REGULAR((STEPS + 1,)),
            pltpu.SemaphoreType.DMA((2, STEPS)),
            pltpu.SemaphoreType.DMA((2,)),
            pltpu.SemaphoreType.DMA((2,)),
            pltpu.SemaphoreType.DMA((3, 4)),
            pltpu.SemaphoreType.DMA((3, 4)),
            pltpu.SemaphoreType.DMA((3,)),
            pltpu.SemaphoreType.DMA((3,)),
            pltpu.SemaphoreType.DMA((3,)),
            pltpu.SemaphoreType.DMA((3,)),
            pltpu.SemaphoreType.DMA,
            pltpu.SemaphoreType.DMA,
            pltpu.SemaphoreType.DMA,
            pltpu.SemaphoreType.DMA((3,)),
        ],
        compiler_params=pltpu.CompilerParams(
            collective_id=0, has_side_effects=True, vmem_limit_bytes=60 * 2**20
        ),
    )(right_side, diagonal, regime, inverses.reshape(NREG * DEEP, DEEP))
    slab = pltpu.VMEM(right_side.shape, f32)
    groups = SLAB // GROUP
    return pl.pallas_call(
        residual_kernel,
        out_shape=(shape, shape),
        in_specs=[anywhere] * 6 + [pl.BlockSpec(memory_space=pltpu.VMEM)],
        out_specs=[anywhere] * 2,
        scratch_shapes=[
            pltpu.VMEM(wide, f32), pltpu.VMEM(few, f32), slab, slab, slab,
            pltpu.VMEM((4, SLAB, LANES), f32),
            pltpu.VMEM((2, SLAB, LANES), f32),
            pltpu.VMEM((LANES, LANES), f32),
            pltpu.VMEM((ROWS, LANES), f32),
            pltpu.SemaphoreType.DMA((9, groups + 1)),
            pltpu.SemaphoreType.DMA((2, groups)),
        ],
        compiler_params=pltpu.CompilerParams(vmem_limit_bytes=60 * 2**20),
    )(right_side, diagonal, inner, terms, sides, ends, weights)


def solution(mesh):
    field = P("gz", "gx", "gy")
    return jax.shard_map(
        per_device,
        mesh=mesh,
        in_specs=(field, field, P("gx", "gy"), P()),
        out_specs=(field, field),
        check_vma=False,
    )
```
